32 devices in a mesh: utt: 4 (over z), tm: 8 (over y, x, core).
Axes of the slice: x: 2, y: 2, z: 4, core: 2. Of those that a mesh axis runs over, the one named last changes fastest.
Arguments:
- inputs: bfloat16 [4, 8192, 512], P('utt', 'tm'), may hold values from -6 to 6
- cotangent: bfloat16 [4, 8192, 512], P('utt', 'tm'), may hold values from -6 to 6
- frame_mask: int32 [4, 8192], P('utt', 'tm'), may hold values from 0 to 1, as said below
- slot_lengths: int32 [4, 4], P('utt'), may hold values from 1024 to 3072, as said below
- decays: float32 [4, 8, 8192], P('utt', None, 'tm'), may hold values from 0.0005 to 1
- tile_slots: int32 [22], replicated, may hold values from 0 to 31, as said below
- master_weight_tiles: float32 [2048, 8, 512], P(('utt', 'tm')), may hold values from -6 to 6
- tile_first: float32 [2048, 8, 512], P(('utt', 'tm'))
- tile_second: float32 [2048, 8, 512], P(('utt', 'tm'))
- vector_master: float32 [27, 512], replicated
- vector_first: float32 [27, 512], replicated
- vector_second: float32 [27, 512], replicated
Outputs:
- output: bfloat16 [4, 8192, 512], P('utt', 'tm')
- grad_input: float32 [4, 8192, 512], P('utt', 'tm')
- new_tile_master: float32 [2048, 8, 512], P(('utt', 'tm'))
- new_tile_first: float32 [2048, 8, 512], P(('utt', 'tm'))
- new_tile_second: float32 [2048, 8, 512], P(('utt', 'tm'))
- tile_copy: bfloat16 [2048, 8, 512], P(('utt', 'tm'))
- new_vector_master: float32 [27, 512], replicated
- new_vector_first: float32 [27, 512], replicated
- new_vector_second: float32 [27, 512], replicated
The draws below stay inside these ranges and needn't reach their ends.
Inputs may be any that keep to these rules, and one draw needn't show every extreme that they name: `slot_lengths`: the 4 slots of a group lie end to end in order and fill its 8192 frames; every group has a slot of 3072 frames and one of 1024. `frame_mask`: within each slot the 1s come first and cover at least three quarters of it; every group has a slot that is 1 throughout and one that is not. `tile_slots`: 22 distinct slots; slot s belongs to the owner s // 8; every slot of some owner is used.
All inputs are finite; a program needn't handle non-finite values.
Results may differ from the reference program's by a relative error of at most 0.015.
Values may be sent and summed in bfloat16 or wider, within the bound.
A program may use at most 256 MiB of HBM per device.

```python
import math
import jax
import jax.numpy as jnp
from jax import lax

D = 512
FF = 2048
H = 8
NS = 32
K = 15
CHIP_TIME_STEPS = 1024
BLK = 512
STEP = 7
P_SIZE = 64
SPOKEN_BATCHES = 4
BATCH_TIME_STEPS = 8192
SLOTS = 4
TOTAL = 32768
NTILE = 22
CAP = 8
NVEC = 27


def slot_layout(key):
    base_length = 2 * CHIP_TIME_STEPS
    reach_frames = CHIP_TIME_STEPS
    half_count = SLOTS // 2
    offsets = jax.random.randint(jax.random.fold_in(key, 21), (SPOKEN_BATCHES, half_count), 0, reach_frames + 1)
    offsets = offsets.at[:, 0].set(reach_frames)
    lengths_all = jnp.concatenate([base_length + offsets, base_length - offsets], axis=1)
    dropped = jax.random.randint(jax.random.fold_in(key, 22), (SPOKEN_BATCHES, SLOTS), 0, lengths_all // 4 + 1)
    dropped = dropped.at[:, 0].set(0)
    dropped = dropped.at[:, half_count].set(lengths_all[:, half_count] // 4)
    live_frames = lengths_all - dropped
    shuffle = jax.vmap(lambda part_key: jax.random.permutation(part_key, SLOTS))(jax.random.split(jax.random.fold_in(key, 23), SPOKEN_BATCHES))
    lengths_out = jnp.take_along_axis(lengths_all, shuffle, axis=1).astype(jnp.int32)
    live_out = jnp.take_along_axis(live_frames, shuffle, axis=1).astype(jnp.int32)
    return (lengths_out, live_out)


def draw_slot_lengths(key, part):
    return slot_layout(key)[0]


def draw_frame_mask(key, part):
    lengths_all, live_frames = slot_layout(key)
    starts = jnp.cumsum(lengths_all, axis=1) - lengths_all
    positions = jnp.arange(BATCH_TIME_STEPS, dtype=jnp.int32)
    inside = (positions[None, :, None] >= starts[:, None, :]) & (positions[None, :, None] < (starts + live_frames)[:, None, :])
    return jnp.any(inside, axis=2).astype(jnp.int32)


def slot_choice(key):
    full_owner = jax.random.randint(jax.random.fold_in(key, 41), (), 0, SPOKEN_BATCHES)
    spare = (SPOKEN_BATCHES - 1) * CAP
    others = jnp.arange(spare, dtype=jnp.int32)
    others = others + CAP * (others >= full_owner * CAP).astype(jnp.int32)
    ranking = jax.random.permutation(jax.random.fold_in(key, 42), spare)
    last_slot = SPOKEN_BATCHES * CAP - 1
    priority = jnp.where((others == 0) | (others == last_slot), ranking - spare, ranking)
    picked = others[jnp.argsort(priority)][:NTILE - CAP]
    full_slots = full_owner * CAP + jnp.arange(CAP, dtype=jnp.int32)
    chosen = jnp.concatenate([full_slots, picked])
    return jax.random.permutation(jax.random.fold_in(key, 43), chosen).astype(jnp.int32)


def draw_tile_slots(key, part):
    return slot_choice(key)


def draw_master_weight_tiles(key, part):
    slots_drawn = slot_choice(key)
    blocks_ff = FF // D
    offset = 2 * blocks_ff
    scales = jnp.full((NTILE,), D ** (-0.5), jnp.float32)
    scales = scales.at[blocks_ff:offset].set(FF ** (-0.5))
    scales = scales.at[offset + 6 + blocks_ff:].set(FF ** (-0.5))
    scales = scales.at[offset].set(0.05 * D ** (-0.5))
    scales = scales.at[offset + 1].set(0.13 * D ** (-0.5))
    scales = scales.at[offset + 2].set(0.11 * D ** (-0.5))
    slot_scales = jnp.full((SPOKEN_BATCHES * CAP,), D ** (-0.5), jnp.float32).at[slots_drawn].set(scales)
    normals = jnp.clip(jax.random.normal(jax.random.fold_in(key, 51), (SPOKEN_BATCHES, D, CAP, D), jnp.float32), -6.0, 6.0)
    return (normals * slot_scales.reshape(SPOKEN_BATCHES, 1, CAP, 1)).reshape(SPOKEN_BATCHES * D, CAP, D)


def draw_tile_first(key, part):
    normals = jnp.clip(jax.random.normal(jax.random.fold_in(key, 61), (SPOKEN_BATCHES * D, CAP, D), jnp.float32), -6.0, 6.0)
    return normals * (0.022 * math.sqrt(TOTAL))


def draw_tile_second(key, part):
    spread = jax.random.uniform(jax.random.fold_in(key, 62), (SPOKEN_BATCHES * D, CAP, D), jnp.float32, math.log(0.5), math.log(4.0))
    return jnp.exp(spread) * (9e-05 * TOTAL)


def draw_vector_master(key, part):
    gain_rows = 1.0 + 0.25 * jax.random.uniform(jax.random.fold_in(key, 71), (6, D), jnp.float32, -1.0, 1.0)
    shift_rows = 0.3 * jnp.clip(jax.random.normal(jax.random.fold_in(key, 72), (6, D), jnp.float32), -4.0, 4.0)
    tap_rows = K ** (-0.5) * jnp.clip(jax.random.normal(jax.random.fold_in(key, 73), (K, D), jnp.float32), -4.0, 4.0)
    return jnp.concatenate([gain_rows, shift_rows, tap_rows], axis=0)


def draw_vector_first(key, part):
    normals = jnp.clip(jax.random.normal(jax.random.fold_in(key, 74), (NVEC, D), jnp.float32), -6.0, 6.0)
    return normals * (0.055 * math.sqrt(TOTAL))


def draw_vector_second(key, part):
    spread = jax.random.uniform(jax.random.fold_in(key, 75), (NVEC, D), jnp.float32, math.log(0.0005), math.log(0.008))
    return jnp.exp(spread) * (0.25 * TOTAL)


def draw_decays(key, part):
    fast_share = 0.5
    is_fast = jax.random.uniform(jax.random.fold_in(key, 31), (SPOKEN_BATCHES, H, 1), jnp.float32) < fast_share
    fast_rate = jnp.exp(jax.random.uniform(jax.random.fold_in(key, 32), (SPOKEN_BATCHES, H, 1), jnp.float32, math.log(20.0), math.log(35.0))) / CHIP_TIME_STEPS
    slow_rate = jnp.exp(jax.random.uniform(jax.random.fold_in(key, 33), (SPOKEN_BATCHES, H, 1), jnp.float32, math.log(0.1), math.log(0.4))) * math.log(10.0) / (3 * CHIP_TIME_STEPS)
    base_rate = jnp.where(is_fast, fast_rate, slow_rate)
    device_count = BATCH_TIME_STEPS // CHIP_TIME_STEPS
    device_factor = jnp.exp(jax.random.uniform(jax.random.fold_in(key, 34), (SPOKEN_BATCHES, H, device_count, 1), jnp.float32, math.log(0.5), math.log(2.0)))
    device_factor = jnp.broadcast_to(device_factor, (SPOKEN_BATCHES, H, device_count, CHIP_TIME_STEPS)).reshape(SPOKEN_BATCHES, H, BATCH_TIME_STEPS)
    frame_factor = jnp.exp(jax.random.uniform(jax.random.fold_in(key, 35), (SPOKEN_BATCHES, H, BATCH_TIME_STEPS), jnp.float32, math.log(0.7), math.log(1.4)))
    averaging_coefficient = jnp.exp(-base_rate * device_factor * frame_factor)
    spell_span = jax.random.randint(jax.random.fold_in(key, 36), (SPOKEN_BATCHES, 1, BATCH_TIME_STEPS), 0, CHIP_TIME_STEPS) == 0
    stack_count = jax.random.uniform(jax.random.fold_in(key, 37), (SPOKEN_BATCHES, H, BATCH_TIME_STEPS), jnp.float32, 0.5, 0.8)
    return jnp.where(spell_span, averaging_coefficient * stack_count, averaging_coefficient)


def levels(own_key, shape, shards, smallest, high):
    def one(position, shards_of):
        draws = jax.random.uniform(jax.random.fold_in(jax.random.fold_in(own_key, 6), position), (shards_of,), jnp.float32, smallest / len(shards), high / len(shards))
        return jnp.repeat(jnp.exp(draws), shape[position] // shards_of).reshape((-1,) + (1,) * (len(shape) - position - 1))

    loudness = one(*shards[0])
    for cut in shards[1:]:
        loudness = loudness * one(*cut)
    return loudness


def scatter_about(rng, dims, scale, most, pieces=(), kind=jnp.bfloat16):
    drawn = scale * jax.random.normal(rng, dims, jnp.float32)
    if pieces:
        drawn = drawn * levels(rng, dims, pieces, -0.22, 0.18)
    return jnp.clip(drawn, -most, most).astype(kind)


def setup_inputs(seed: int = 0) -> dict:
    keys = jax.random.split(jax.random.key(seed), 13)
    inputs = scatter_about(keys[0], (SPOKEN_BATCHES, BATCH_TIME_STEPS, D), 1.0, 6.0, ((0, 4), (1, 8)))
    cotangent = scatter_about(keys[1], (SPOKEN_BATCHES, BATCH_TIME_STEPS, D), 1.0, 6.0, ((0, 4), (1, 8)))
    frame_mask = draw_frame_mask(jax.random.fold_in(keys[12], 71), 0)
    slot_lengths = draw_slot_lengths(jax.random.fold_in(keys[12], 71), 0)
    decays = draw_decays(jax.random.fold_in(keys[12], 71), 0)
    tile_slots = draw_tile_slots(jax.random.fold_in(keys[12], 71), 0)
    master_weight_tiles = draw_master_weight_tiles(jax.random.fold_in(keys[12], 71), 0)
    tile_first = draw_tile_first(jax.random.fold_in(keys[12], 71), 0)
    tile_second = draw_tile_second(jax.random.fold_in(keys[12], 71), 0)
    vector_master = draw_vector_master(jax.random.fold_in(keys[12], 71), 0)
    vector_first = draw_vector_first(jax.random.fold_in(keys[12], 71), 0)
    vector_second = draw_vector_second(jax.random.fold_in(keys[12], 71), 0)
    return dict(inputs=inputs, cotangent=cotangent, frame_mask=frame_mask, slot_lengths=slot_lengths, decays=decays, tile_slots=tile_slots, master_weight_tiles=master_weight_tiles, tile_first=tile_first, tile_second=tile_second, vector_master=vector_master, vector_first=vector_first, vector_second=vector_second)


NORM_EPS = 1e-05
ADAM_EPS = 1e-08
BETA_ONE = 0.9
BETA_TWO = 0.999
RATE_TILES = 0.04
RATE_VECTORS = 0.1
DECAY_TILES = 0.1
PRECISE = lax.Precision.HIGHEST

@jax.custom_vjp
def low(v):
    return lax.optimization_barrier(v.astype(jnp.bfloat16)).astype(jnp.float32)

@jax.custom_vjp
def low_back(v):
    return v

def low_keep(v):
    return (low(v), None)

def low_pass(kept, grad):
    return (grad,)

def back_keep(v):
    return (v, None)

def back_low(kept, grad):
    return (low(grad),)
low.defvjp(low_keep, low_pass)
low_back.defvjp(back_keep, back_low)

def matmul_exact(matrix_a, matrix_b):
    return jnp.dot(matrix_a, matrix_b, precision=PRECISE)

def layer_norm(values, norm_gain, norm_shift):
    centered = values - lax.optimization_barrier(jnp.mean(values, axis=-1, keepdims=True))
    inverse_dev = lax.rsqrt(lax.optimization_barrier(jnp.mean(centered * centered, axis=-1, keepdims=True)) + NORM_EPS)
    return centered * inverse_dev * norm_gain + norm_shift

def segment_ids(lengths, frames):
    starts = (jnp.cumsum(lengths) - lengths).astype(jnp.int32)
    positions = jnp.arange(frames, dtype=jnp.int32)
    return (lax.optimization_barrier(jnp.sum((starts[None, :] <= positions[:, None]).astype(jnp.int32), axis=1)) - 1).astype(jnp.int32)

def split_tiles(tile_values):
    blocks_ff = FF // D
    offset = 2 * blocks_ff
    up_first = tile_values[0:blocks_ff].transpose(1, 0, 2).reshape(D, FF)
    down_first = tile_values[blocks_ff:offset].reshape(FF, D)
    mixers = [tile_values[offset + number] for number in range(6)]
    up_second = tile_values[offset + 6:offset + 6 + blocks_ff].transpose(1, 0, 2).reshape(D, FF)
    down_second = tile_values[offset + 6 + blocks_ff:offset + 6 + 2 * blocks_ff].reshape(FF, D)
    return (up_first, down_first, mixers, up_second, down_second)

def half_ffn(values, w_up, w_down, norm_gain, norm_shift):
    normed = low(layer_norm(values, norm_gain, norm_shift))
    hidden = low_back(matmul_exact(normed, w_up))
    activated = low(hidden * jax.nn.sigmoid(hidden))
    return values + 0.5 * low_back(matmul_exact(activated, w_down))

def state_block(run_state, block_item):
    queries, state_keys, state_vals, log_piece, seg_piece, seg_prior = block_item
    cumulative = jnp.cumsum(log_piece, axis=1)
    row_index = jnp.arange(seg_piece.shape[0], dtype=jnp.int32)
    allowed = (seg_piece[:, None] == seg_piece[None, :]) & (row_index[:, None] >= row_index[None, :])
    exponent = jnp.where(allowed[None], cumulative[:, :, None] - cumulative[:, None, :], 0.0)
    within = jnp.where(allowed[None], jnp.exp(exponent), 0.0)
    entering = jnp.where((seg_piece == seg_prior)[None, :], jnp.exp(cumulative), 0.0)
    leaving = jnp.where((seg_piece == seg_piece[-1])[None, :], jnp.exp(cumulative[:, -1:] - cumulative), 0.0)
    scores = low_back(jnp.einsum('thn,shn->hts', queries, state_keys, precision=PRECISE))
    mixed_low = low(within * scores)
    inner_part = jnp.einsum('hts,shp->thp', mixed_low, state_vals, precision=PRECISE)
    carried = jnp.einsum('thn,hnp->thp', queries * entering.T[:, :, None], run_state, precision=PRECISE)
    new_state = jnp.einsum('shn,shp->hnp', state_keys * leaving.T[:, :, None], state_vals, precision=PRECISE)
    new_state = new_state + entering[:, -1][:, None, None] * run_state
    return (new_state, inner_part + carried)

def state_mixer(values, w_values, w_states, w_output, norm_gain, norm_shift, live_mask, segments, log_decay):
    frames = values.shape[0]
    block_count = frames // BLK
    normed = low(layer_norm(values, norm_gain, norm_shift))
    state_vals = live_mask[:, None] * low(low_back(matmul_exact(normed, w_values)))
    key_query = low(low_back(matmul_exact(normed, w_states)))
    state_keys = key_query[:, :H * NS].reshape(block_count, BLK, H, NS)
    queries = key_query[:, H * NS:].reshape(block_count, BLK, H, NS)
    state_vals = state_vals.reshape(block_count, BLK, H, P_SIZE)
    log_blocks = log_decay.reshape(H, block_count, BLK).transpose(1, 0, 2)
    seg_blocks = segments.reshape(block_count, BLK)
    priors = jnp.concatenate([jnp.full((1,), -1, jnp.int32), segments[BLK - 1:frames - 1:BLK]]).astype(jnp.int32)
    start_state = jnp.zeros((H, NS, P_SIZE), jnp.float32)
    final_state, outputs = lax.scan(jax.checkpoint(state_block), start_state, (queries, state_keys, state_vals, log_blocks, seg_blocks, priors))
    mixed_out = low(low_back(outputs.reshape(frames, H * P_SIZE)))
    return values + low_back(matmul_exact(mixed_out, w_output))

def conv_module(values, w_linear, w_gate, w_project, vectors, segments):
    frames = values.shape[0]
    half_width = K // 2
    normed = low(layer_norm(values, vectors[2], vectors[8]))
    part_lin = low_back(matmul_exact(normed, w_linear))
    part_gate = low_back(matmul_exact(normed, w_gate))
    glu_low = low(part_lin * jax.nn.sigmoid(part_gate))
    padded = jnp.pad(glu_low, ((half_width, half_width), (0, 0)))
    pad_segments = jnp.pad(segments, (half_width, half_width), constant_values=-1)
    conv_sum = jnp.zeros(values.shape, jnp.float32)
    for kernel_offset in range(K):
        same_mask = (pad_segments[kernel_offset:kernel_offset + frames] == segments).astype(jnp.float32)
        conv_sum = conv_sum + vectors[12 + kernel_offset] * padded[kernel_offset:kernel_offset + frames] * same_mask[:, None]
    conv_sum = low_back(conv_sum)
    normed_inner = layer_norm(conv_sum, vectors[3], vectors[9])
    activated = low(normed_inner * jax.nn.sigmoid(normed_inner))
    return values + low_back(matmul_exact(activated, w_project))

def group_forward(tile_values, vectors, start_x, live_mask, segments, log_decay):
    up_first, down_first, mixers, up_second, down_second = split_tiles(tile_values)
    after_a = half_ffn(start_x, up_first, down_first, vectors[0], vectors[6])
    after_b = state_mixer(after_a, mixers[0], mixers[1], mixers[2], vectors[1], vectors[7], live_mask, segments, log_decay)
    after_c = conv_module(after_b, mixers[3], mixers[4], mixers[5], vectors, segments)
    after_e = half_ffn(after_c, up_second, down_second, vectors[4], vectors[10])
    return layer_norm(after_e, vectors[5], vectors[11])

def adam_step(master, first_old, second, gradient, step_rate, decay_rate):
    first_new = BETA_ONE * first_old + (1.0 - BETA_ONE) * gradient
    second_new = BETA_TWO * second + (1.0 - BETA_TWO) * gradient * gradient
    first_hat = first_new / (1.0 - BETA_ONE ** STEP)
    second_hat = second_new / (1.0 - BETA_TWO ** STEP)
    master_new = master - step_rate * (first_hat / (jnp.sqrt(second_hat) + ADAM_EPS) + decay_rate * master)
    return (master_new, first_new, second_new)

def reference(inputs, cotangent, frame_mask, slot_lengths, decays, tile_slots, master_weight_tiles, tile_first, tile_second, vector_master, vector_first, vector_second):
    owners = master_weight_tiles.shape[0] // D
    capacity = master_weight_tiles.shape[1]
    grouped = master_weight_tiles.reshape(owners, D, capacity, D)
    owner_of = (tile_slots // capacity).astype(jnp.int32)
    column_of = (tile_slots % capacity).astype(jnp.int32)
    tile_values = low(grouped[owner_of, :, column_of, :])

    def one_group(totals, group_item):
        group_x, group_cot, group_mask, batch_spans, group_decay = group_item
        frames = group_x.shape[0]
        segments = segment_ids(batch_spans, frames)
        live_mask = group_mask.astype(jnp.float32)
        log_decay = jnp.log(group_decay)

        def forward(tile_arg, vector_arg, start_x):
            return group_forward(tile_arg, vector_arg, start_x, live_mask, segments, log_decay)
        result, pullback = jax.vjp(forward, tile_values, vector_master, group_x.astype(jnp.float32))
        grad_tiles, grad_vectors, grad_x = pullback(group_cot.astype(jnp.float32))
        return ((totals[0] + grad_tiles, totals[1] + grad_vectors), (result.astype(jnp.bfloat16), grad_x))
    zeros_start = (jnp.zeros(tile_values.shape, jnp.float32), jnp.zeros(vector_master.shape, jnp.float32))
    totals, per_group = lax.scan(one_group, zeros_start, (inputs, cotangent, frame_mask, slot_lengths, decays))
    grad_tiles, grad_vectors = totals
    output, grad_input = per_group
    buffer = jnp.zeros((owners, D, capacity, D), jnp.float32).at[owner_of, :, column_of, :].set(grad_tiles)
    buffer = buffer.reshape(owners * D, capacity, D)
    tile_new, first_new, second_new = adam_step(master_weight_tiles, tile_first, tile_second, buffer, RATE_TILES, DECAY_TILES)
    vector_new, vfirst_new, vsecond_new = adam_step(vector_master, vector_first, vector_second, grad_vectors, RATE_VECTORS, 0.0)
    return (output, grad_input, tile_new, first_new, second_new, tile_new.astype(jnp.bfloat16), vector_new, vfirst_new, vsecond_new)
```

```python
import jax
import jax.numpy as jnp
from jax import lax
from jax.sharding import PartitionSpec as P

D = 512
FF = 2048
H = 8
NS = 32
K = 15
BLK = 512
STEP = 7
P_SIZE = 64


NORM_EPS = 1e-05
ADAM_EPS = 1e-08
BETA_ONE = 0.9
BETA_TWO = 0.999
RATE_TILES = 0.04
RATE_VECTORS = 0.1
DECAY_TILES = 0.1
PRECISE = lax.Precision.HIGHEST


def entering_2(shard, axis, join, neutral, backward):
    count = lax.axis_size(axis)
    place = lax.axis_index(axis)
    ahead = count - 1 - place if backward else place
    gathered = jax.tree.map(
        lambda a, kind: lax.all_gather(a.astype(kind), axis), shard, (jnp.bfloat16, jnp.bfloat16)
    )
    state = jax.tree.map(lambda a, e: jnp.zeros_like(a) + jnp.asarray(e, a.dtype), shard, neutral)

    def one(lap, state):
        source = count - 1 - lap if backward else lap
        return join(
            state,
            jax.tree.map(
                lambda a, own: lax.dynamic_index_in_dim(a, source, 0, False).astype(own.dtype),
                gathered,
                shard,
            ),
        )

    return lax.fori_loop(0, ahead, one, state)


def padded_2(cells, sides, width):
    for axis, dim in sides:
        count = lax.axis_size(axis)
        ends = count - 1
        head = lax.slice_in_dim(cells, 0, width, axis=dim)
        tail = lax.slice_in_dim(cells, cells.shape[dim] - width, cells.shape[dim], axis=dim)
        cells = jnp.concatenate(
            [
                lax.ppermute(tail, axis, [(i, (i + 1) % count) for i in range(ends)]),
                cells,
                lax.ppermute(head, axis, [((i + 1) % count, i) for i in range(ends)]),
            ],
            axis=dim,
        )
    return cells


def product(matrix_a, matrix_b):
    return jnp.dot(matrix_a, matrix_b, preferred_element_type=jnp.float32)


def weight_grad(activations, gradients):
    return lax.dot_general(
        activations, gradients, (((0,), (0,)), ((), ())), preferred_element_type=jnp.float32
    )


def input_grad(gradients, weights):
    return lax.dot_general(
        gradients, weights, (((1,), (1,)), ((), ())), preferred_element_type=jnp.float32
    )


def layer_norm(values, norm_gain, norm_shift):
    centered = values - jnp.mean(values, axis=-1, keepdims=True)
    inverse_dev = lax.rsqrt(jnp.mean(centered * centered, axis=-1, keepdims=True) + NORM_EPS)
    normed = centered * inverse_dev
    return (normed * norm_gain + norm_shift, normed, inverse_dev)


def norm_grad(gradients, normed, inverse_dev, norm_gain):
    scaled = gradients * norm_gain
    middle = (
        scaled
        - jnp.mean(scaled, axis=-1, keepdims=True)
        - normed * jnp.mean(scaled * normed, axis=-1, keepdims=True)
    )
    return (middle * inverse_dev, jnp.sum(gradients * normed, axis=0), jnp.sum(gradients, axis=0))


def swish_slope(pre_act):
    sigmoid_of = jax.nn.sigmoid(pre_act)
    return sigmoid_of * (1.0 + pre_act * (1.0 - sigmoid_of))


def split_tiles(tile_values):
    blocks_ff = FF // D
    offset = 2 * blocks_ff
    up_first = tile_values[0:blocks_ff].transpose(1, 0, 2).reshape(D, FF)
    down_first = tile_values[blocks_ff:offset].reshape(FF, D)
    mixers = [tile_values[offset + number] for number in range(6)]
    up_second = tile_values[offset + 6 : offset + 6 + blocks_ff].transpose(1, 0, 2).reshape(D, FF)
    down_second = tile_values[offset + 6 + blocks_ff : offset + 6 + 2 * blocks_ff].reshape(FF, D)
    return (up_first, down_first, mixers, up_second, down_second)


def column_tiles(full_grad):
    blocks_ff = FF // D
    return full_grad.reshape(D, blocks_ff, D).transpose(1, 0, 2)


def ffn_forward(start_x, up_weight, down_weight, norm_gain, norm_shift):
    normed_out, normed, inverse_dev = layer_norm(start_x, norm_gain, norm_shift)
    normed_low = normed_out.astype(jnp.bfloat16)
    hidden = product(normed_low, up_weight)
    activated = (hidden * jax.nn.sigmoid(hidden)).astype(jnp.bfloat16)
    return (
        start_x + 0.5 * product(activated, down_weight),
        (normed, inverse_dev, normed_low, hidden, activated),
    )


def ffn_backward(grad_after, kept, up_weight, down_weight, norm_gain):
    normed, inverse_dev, normed_low, hidden, activated = kept
    down_in = (0.5 * grad_after).astype(jnp.bfloat16)
    grad_down = weight_grad(activated, down_in)
    hidden_grad = (input_grad(down_in, down_weight) * swish_slope(hidden)).astype(jnp.bfloat16)
    grad_up = weight_grad(normed_low, hidden_grad)
    grad_normed, gain_grad, shift_grad = norm_grad(
        input_grad(hidden_grad, up_weight), normed, inverse_dev, norm_gain
    )
    return (grad_after + grad_normed, grad_up, grad_down, gain_grad, shift_grad)


def block_weights(log_piece, seg_piece, seg_prior):
    cumulative = jnp.cumsum(log_piece, axis=1)
    row_index = jnp.arange(seg_piece.shape[0], dtype=jnp.int32)
    allowed = (seg_piece[:, None] == seg_piece[None, :]) & (
        row_index[:, None] >= row_index[None, :]
    )
    exponent = jnp.where(allowed[None], cumulative[:, :, None] - cumulative[:, None, :], 0.0)
    within = jnp.where(allowed[None], jnp.exp(exponent), 0.0)
    entering = jnp.where((seg_piece == seg_prior)[None, :], jnp.exp(cumulative), 0.0)
    leaving = jnp.where(
        (seg_piece == seg_piece[-1])[None, :], jnp.exp(cumulative[:, -1:] - cumulative), 0.0
    )
    return (within, entering, leaving)


def chain_states(earlier, latter):
    return (latter[0] * earlier[0], latter[0][:, None, None] * earlier[1] + latter[1])


def adam_step(master, first_old, second, gradient, step_rate, decay_rate):
    first_new = BETA_ONE * first_old + (1.0 - BETA_ONE) * gradient
    second_new = BETA_TWO * second + (1.0 - BETA_TWO) * gradient * gradient
    first_hat = first_new / (1.0 - BETA_ONE**STEP)
    second_hat = second_new / (1.0 - BETA_TWO**STEP)
    master_new = master - step_rate * (
        first_hat / (jnp.sqrt(second_hat) + ADAM_EPS) + decay_rate * master
    )
    return (master_new, first_new, second_new)


def halving_sum(cells, axis):
    bits = lax.axis_size(axis).bit_length() - 1
    count = cells.shape[1]
    cells = exchange_bit(cells, axis, 0, 0)
    parts = []
    for piece, order in (
        (cells[:, : count // 2], list(range(bits - 1))),
        (cells[:, count // 2 :], list(reversed(range(bits - 1)))),
    ):
        left = list(range(bits - 1))
        for bit in order:
            place = left.index(bit)
            piece = exchange_bit(piece, axis, place, bit + 1)
            left.remove(bit)
        parts.append(piece[0])
    return jnp.concatenate(parts, axis=0)


def exchange_bit(cells, axis, place, bit):
    count = lax.axis_size(axis)
    mine = (lax.axis_index(axis) >> bit) & 1
    shape = cells.shape
    cells = cells.reshape(shape[0] >> (place + 1), 2, 1 << place, *shape[1:])
    kept = lax.dynamic_index_in_dim(cells, mine, 1, False)
    sent = lax.dynamic_index_in_dim(cells, 1 - mine, 1, False)
    got = lax.ppermute(sent, axis, [(i, i ^ (1 << bit)) for i in range(count)])
    total = (kept.astype(jnp.float32) + got.astype(jnp.float32)).astype(cells.dtype)
    return total.reshape(shape[0] // 2, *shape[1:])


def local(
    inputs,
    cotangent,
    frame_mask,
    slot_lengths,
    decays,
    tile_slots,
    master_weight_tiles,
    tile_first,
    tile_second,
    vector_master,
    vector_first,
    vector_second,
):
    own_rows, capacity, _ = master_weight_tiles.shape
    owners_count = lax.axis_size("utt")
    low_master = master_weight_tiles.transpose(1, 0, 2).astype(jnp.bfloat16)
    by_slot = lax.all_gather(low_master, "utt", axis=0, tiled=True)
    chosen = by_slot[tile_slots]
    groups = []
    for first, last in ((0, 8), (8, 22)):
        part = lax.all_gather(chosen[first:last], "tm", axis=0)
        groups.append(part.transpose(1, 0, 2, 3).reshape(last - first, D, D))
    tile_values = jnp.concatenate(groups, axis=0)
    up_first, down_first, mixers, up_second, down_second = split_tiles(tile_values)
    w_values, w_states, w_output, w_linear, w_gate, w_project = mixers
    norm_gains = vector_master[0:6]
    norm_shifts = vector_master[6:12]
    conv_taps = vector_master[12:]
    frames = inputs.shape[1]
    first_frame = lax.axis_index("tm") * frames
    starts = jnp.cumsum(slot_lengths[0]) - slot_lengths[0]

    def segment_of(positions):
        return jnp.sum((starts[None, :] <= positions[:, None]).astype(jnp.int32), axis=1) - 1

    positions = first_frame + jnp.arange(frames, dtype=jnp.int32)
    segments = segment_of(positions)
    seg_before = segment_of(jnp.reshape(first_frame - 1, (1,)))[0]
    log_decay = jnp.log(decays[0])
    start_x = inputs[0].astype(jnp.float32)
    after_a, kept_a = ffn_forward(start_x, up_first, down_first, norm_gains[0], norm_shifts[0])
    normed_b_out, unit_b, inverse_b = layer_norm(after_a, norm_gains[1], norm_shifts[1])
    low_b = normed_b_out.astype(jnp.bfloat16)
    live_mask = frame_mask[0].astype(jnp.bfloat16)[:, None]
    state_vals = (product(low_b, w_values).astype(jnp.bfloat16) * live_mask).reshape(
        frames, H, P_SIZE
    )
    key_query = product(low_b, w_states).astype(jnp.bfloat16)
    state_keys = key_query[:, : H * NS].reshape(frames, H, NS)
    state_query = key_query[:, H * NS :].reshape(frames, H, NS)
    keys_wide = state_keys.astype(jnp.float32)
    query_wide = state_query.astype(jnp.float32)
    vals_wide = state_vals.astype(jnp.float32)
    total_log = jnp.cumsum(log_decay, axis=1)
    tail_dev = jnp.where(
        (segments == segments[-1])[None, :], jnp.exp(total_log[:, -1:] - total_log), 0.0
    )
    local_state = jnp.einsum(
        "shn,shp->hnp", keys_wide * tail_dev.T[:, :, None], vals_wide, precision=PRECISE
    )
    carry_dev = jnp.where(segments[-1] == seg_before, jnp.exp(total_log[:, -1]), 0.0)
    identity = (jnp.ones((H,), jnp.float32), jnp.zeros((H, NS, P_SIZE), jnp.float32))
    entry_scale, entry_state = entering_2(
        (carry_dev, local_state), "tm", chain_states, identity, False
    )
    count_blocks = frames // BLK
    saved_blocks = []
    outputs = []
    run_state = entry_state
    for number in range(count_blocks):
        block_start = number * BLK
        rows_here = slice(block_start, block_start + BLK)
        if number == 0:
            seg_prior = seg_before
        else:
            seg_prior = segments[block_start - 1]
        within, entering, leaving = block_weights(
            log_decay[:, rows_here], segments[rows_here], seg_prior
        )
        scores = jnp.einsum(
            "thn,shn->hts",
            state_query[rows_here],
            state_keys[rows_here],
            preferred_element_type=jnp.float32,
        )
        mixed_low = (within * scores).astype(jnp.bfloat16)
        inner_part = jnp.einsum(
            "hts,shp->thp", mixed_low, state_vals[rows_here], preferred_element_type=jnp.float32
        )
        carried = jnp.einsum(
            "thn,hnp->thp",
            query_wide[rows_here] * entering.T[:, :, None],
            run_state,
            precision=PRECISE,
        )
        outputs.append(inner_part + carried)
        saved_blocks.append((within, entering, leaving, mixed_low, run_state))
        run_state = (
            jnp.einsum(
                "shn,shp->hnp",
                keys_wide[rows_here] * leaving.T[:, :, None],
                vals_wide[rows_here],
                precision=PRECISE,
            )
            + entering[:, -1][:, None, None] * run_state
        )
    low_y = jnp.concatenate(outputs, axis=0).reshape(frames, H * P_SIZE).astype(jnp.bfloat16)
    after_b = after_a + product(low_y, w_output)
    normed_c_out, unit_c, inverse_c = layer_norm(after_b, norm_gains[2], norm_shifts[2])
    low_c = normed_c_out.astype(jnp.bfloat16)
    part_lin = product(low_c, w_linear)
    part_gate = product(low_c, w_gate)
    gate_sigmoid = jax.nn.sigmoid(part_gate)
    glu_low = (part_lin * gate_sigmoid).astype(jnp.bfloat16)
    half_width = K // 2
    padded = padded_2(glu_low, (("tm", 0),), half_width)
    pad_positions = first_frame - half_width + jnp.arange(frames + 2 * half_width, dtype=jnp.int32)
    pad_segments = segment_of(pad_positions)
    tap_masks = [
        (pad_segments[kernel_offset : kernel_offset + frames] == segments).astype(jnp.float32)[
            :, None
        ]
        for kernel_offset in range(K)
    ]
    conv_sum = jnp.zeros((frames, D), jnp.float32)
    for kernel_offset in range(K):
        conv_sum = (
            conv_sum
            + conv_taps[kernel_offset]
            * padded[kernel_offset : kernel_offset + frames].astype(jnp.float32)
            * tap_masks[kernel_offset]
        )
    normed_d, unit_d, inverse_d = layer_norm(conv_sum, norm_gains[3], norm_shifts[3])
    low_d = (normed_d * jax.nn.sigmoid(normed_d)).astype(jnp.bfloat16)
    after_c = after_b + product(low_d, w_project)
    after_e, kept_e = ffn_forward(after_c, up_second, down_second, norm_gains[4], norm_shifts[4])
    final_out, unit_f, inverse_f = layer_norm(after_e, norm_gains[5], norm_shifts[5])
    output = final_out.astype(jnp.bfloat16)[None]
    grad_out = cotangent[0].astype(jnp.float32)
    grad_e, gain_f, shift_f = norm_grad(grad_out, unit_f, inverse_f, norm_gains[5])
    grad_c, grad_up_e, grad_down_e, gain_e, shift_e = ffn_backward(
        grad_e, kept_e, up_second, down_second, norm_gains[4]
    )
    project_in = grad_c.astype(jnp.bfloat16)
    grad_project = weight_grad(low_d, project_in)
    grad_swish = input_grad(project_in, w_project) * swish_slope(normed_d)
    grad_conv, gain_d, shift_d = norm_grad(grad_swish, unit_d, inverse_d, norm_gains[3])
    low_grad_conv = grad_conv.astype(jnp.bfloat16)
    grad_padded = padded_2(low_grad_conv, (("tm", 0),), half_width)
    grad_conv_wide = low_grad_conv.astype(jnp.float32)
    grad_glu = jnp.zeros((frames, D), jnp.float32)
    tap_grads = []
    for kernel_offset in range(K):
        back_start = 2 * half_width - kernel_offset
        grad_glu = (
            grad_glu
            + conv_taps[kernel_offset]
            * grad_padded[back_start : back_start + frames].astype(jnp.float32)
            * tap_masks[K - 1 - kernel_offset]
        )
        tap_grads.append(
            jnp.sum(
                grad_conv_wide
                * padded[kernel_offset : kernel_offset + frames].astype(jnp.float32)
                * tap_masks[kernel_offset],
                axis=0,
            )
        )
    grad_lin = (grad_glu * gate_sigmoid).astype(jnp.bfloat16)
    grad_gate = (grad_glu * part_lin * gate_sigmoid * (1.0 - gate_sigmoid)).astype(jnp.bfloat16)
    grad_w_linear = weight_grad(low_c, grad_lin)
    grad_w_gate = weight_grad(low_c, grad_gate)
    grad_in_c, gain_c, shift_c = norm_grad(
        input_grad(grad_lin, w_linear) + input_grad(grad_gate, w_gate),
        unit_c,
        inverse_c,
        norm_gains[2],
    )
    grad_b = grad_c + grad_in_c
    output_in = grad_b.astype(jnp.bfloat16)
    grad_w_output = weight_grad(low_y, output_in)
    grad_y = input_grad(output_in, w_output).astype(jnp.bfloat16).reshape(frames, H, P_SIZE)
    grad_y_wide = grad_y.astype(jnp.float32)
    entering_dev = jnp.where((segments == seg_before)[None, :], jnp.exp(total_log), 0.0)
    local_back = jnp.einsum(
        "thn,thp->hnp", query_wide * entering_dev.T[:, :, None], grad_y_wide, precision=PRECISE
    )
    exit_scale, exit_grad = entering_2((carry_dev, local_back), "tm", chain_states, identity, True)
    incoming = exit_grad
    vals_parts = []
    keys_parts = []
    query_parts = []
    for number in reversed(range(count_blocks)):
        block_start = number * BLK
        rows_here = slice(block_start, block_start + BLK)
        within, entering, leaving, mixed_low, prior_state = saved_blocks[number]
        grad_blk = grad_y[rows_here]
        grad_blk_wide = grad_y_wide[rows_here]
        grad_mixed = jnp.einsum(
            "thp,shp->hts", grad_blk, state_vals[rows_here], preferred_element_type=jnp.float32
        )
        grad_vals = jnp.einsum(
            "hts,thp->shp", mixed_low, grad_blk, preferred_element_type=jnp.float32
        )
        grad_scores = (within * grad_mixed).astype(jnp.bfloat16)
        grad_query = jnp.einsum(
            "hts,shn->thn", grad_scores, state_keys[rows_here], preferred_element_type=jnp.float32
        )
        grad_keys = jnp.einsum(
            "hts,thn->shn", grad_scores, state_query[rows_here], preferred_element_type=jnp.float32
        )
        grad_query = grad_query + entering.T[:, :, None] * jnp.einsum(
            "thp,hnp->thn", grad_blk_wide, prior_state, precision=PRECISE
        )
        grad_vals = grad_vals + jnp.einsum(
            "shn,hnp->shp",
            keys_wide[rows_here] * leaving.T[:, :, None],
            incoming,
            precision=PRECISE,
        )
        grad_keys = grad_keys + leaving.T[:, :, None] * jnp.einsum(
            "shp,hnp->shn", vals_wide[rows_here], incoming, precision=PRECISE
        )
        incoming = (
            jnp.einsum(
                "thn,thp->hnp",
                query_wide[rows_here] * entering.T[:, :, None],
                grad_blk_wide,
                precision=PRECISE,
            )
            + entering[:, -1][:, None, None] * incoming
        )
        vals_parts.insert(0, grad_vals)
        keys_parts.insert(0, grad_keys)
        query_parts.insert(0, grad_query)
    grad_v_low = (
        jnp.concatenate(vals_parts, axis=0).reshape(frames, D) * live_mask.astype(jnp.float32)
    ).astype(jnp.bfloat16)
    grad_kq_low = jnp.concatenate(
        [
            jnp.concatenate(keys_parts, axis=0).reshape(frames, H * NS),
            jnp.concatenate(query_parts, axis=0).reshape(frames, H * NS),
        ],
        axis=1,
    ).astype(jnp.bfloat16)
    grad_w_values = weight_grad(low_b, grad_v_low)
    grad_w_states = weight_grad(low_b, grad_kq_low)
    grad_in_b, gain_b, shift_b = norm_grad(
        input_grad(grad_v_low, w_values) + input_grad(grad_kq_low, w_states),
        unit_b,
        inverse_b,
        norm_gains[1],
    )
    grad_a = grad_b + grad_in_b
    grad_start, grad_up_a, grad_down_a, gain_a, shift_a = ffn_backward(
        grad_a, kept_a, up_first, down_first, norm_gains[0]
    )
    blocks_ff = FF // D
    count = lax.axis_size("tm")

    def reduce_tiles(parts):
        stacked = jnp.concatenate(parts, axis=0).astype(jnp.bfloat16)
        stacked = stacked.reshape(stacked.shape[0], count, own_rows, D).transpose(1, 0, 2, 3)
        return halving_sum(stacked, "tm")

    middle = reduce_tiles([jnp.stack([grad_w_output, grad_w_linear, grad_w_gate])])
    late = reduce_tiles(
        [
            grad_project[None],
            column_tiles(grad_up_e),
            grad_down_e.reshape(blocks_ff, D, D),
        ]
    )
    early = reduce_tiles(
        [
            column_tiles(grad_up_a),
            grad_down_a.reshape(blocks_ff, D, D),
            jnp.stack([grad_w_values, grad_w_states]),
        ]
    )
    shards = jnp.concatenate([early, middle, late, jnp.zeros((1, own_rows, D), jnp.bfloat16)], axis=0)
    tiles = tile_slots.shape[0]
    tile_of = (
        jnp.full((owners_count * capacity,), tiles, jnp.int32)
        .at[tile_slots]
        .set(jnp.arange(tiles, dtype=jnp.int32))
    )
    placed = shards[tile_of].reshape(owners_count, capacity, own_rows, D)
    reduced = lax.psum_scatter(placed, "utt", scatter_dimension=0)
    reduced = reduced.astype(jnp.float32).transpose(1, 0, 2)
    vector_grad = jnp.concatenate(
        [
            jnp.stack(
                [
                    gain_a,
                    gain_b,
                    gain_c,
                    gain_d,
                    gain_e,
                    gain_f,
                    shift_a,
                    shift_b,
                    shift_c,
                    shift_d,
                    shift_e,
                    shift_f,
                ]
            ),
            jnp.stack(tap_grads),
        ],
        axis=0,
    )
    vector_total = lax.psum(vector_grad, ("utt", "tm"))
    tile_new, first_new, second_new = adam_step(
        master_weight_tiles, tile_first, tile_second, reduced, RATE_TILES, DECAY_TILES
    )
    vector_new, vfirst_new, vsecond_new = adam_step(
        vector_master, vector_first, vector_second, vector_total, RATE_VECTORS, 0.0
    )
    return (
        output,
        grad_start[None],
        tile_new,
        first_new,
        second_new,
        tile_new.astype(jnp.bfloat16),
        vector_new,
        vfirst_new,
        vsecond_new,
    )


def solution(mesh):
    in_specs = (
        P("utt", "tm", None),
        P("utt", "tm", None),
        P("utt", "tm"),
        P("utt", None),
        P("utt", None, "tm"),
        P(),
        P(("utt", "tm"), None, None),
        P(("utt", "tm"), None, None),
        P(("utt", "tm"), None, None),
        P(),
        P(),
        P(),
    )
    out_specs = (
        P("utt", "tm", None),
        P("utt", "tm", None),
        P(("utt", "tm"), None, None),
        P(("utt", "tm"), None, None),
        P(("utt", "tm"), None, None),
        P(("utt", "tm"), None, None),
        P(),
        P(),
        P(),
    )
    return jax.shard_map(local, mesh=mesh, in_specs=in_specs, out_specs=out_specs, check_vma=False)
```

```python
import functools

import jax
import jax.numpy as jnp
from jax import lax
from jax.experimental import pallas as pl
from jax.experimental.pallas import tpu as pltpu
from jax.sharding import PartitionSpec as P

D = 512
FF = 2048
H = 8
NS = 32
K = 15
BLK = 512
STEP = 7
P_SIZE = 64


NORM_EPS = 1e-05
ADAM_EPS = 1e-08
BETA_ONE = 0.9
BETA_TWO = 0.999
RATE_TILES = 0.04
RATE_VECTORS = 0.1
DECAY_TILES = 0.1
PRECISE = lax.Precision.HIGHEST


def padded_2(cells, sides, width):
    for axis, dim in sides:
        count = lax.axis_size(axis)
        ends = count - 1
        head = lax.slice_in_dim(cells, 0, width, axis=dim)
        tail = lax.slice_in_dim(cells, cells.shape[dim] - width, cells.shape[dim], axis=dim)
        cells = jnp.concatenate(
            [
                lax.ppermute(tail, axis, [(i, (i + 1) % count) for i in range(ends)]),
                cells,
                lax.ppermute(head, axis, [((i + 1) % count, i) for i in range(ends)]),
            ],
            axis=dim,
        )
    return cells


def product(matrix_a, matrix_b):
    return jnp.dot(matrix_a, matrix_b, preferred_element_type=jnp.float32)


def weight_grad(activations, gradients):
    return lax.dot_general(
        activations, gradients, (((0,), (0,)), ((), ())), preferred_element_type=jnp.float32
    )


def input_grad(gradients, weights):
    return lax.dot_general(
        gradients, weights, (((1,), (1,)), ((), ())), preferred_element_type=jnp.float32
    )


def layer_norm(values, norm_gain, norm_shift):
    centered = values - jnp.mean(values, axis=-1, keepdims=True)
    inverse_dev = lax.rsqrt(jnp.mean(centered * centered, axis=-1, keepdims=True) + NORM_EPS)
    normed = centered * inverse_dev
    return (normed * norm_gain + norm_shift, normed, inverse_dev)


def norm_grad(gradients, normed, inverse_dev, norm_gain):
    scaled = gradients * norm_gain
    middle = (
        scaled
        - jnp.mean(scaled, axis=-1, keepdims=True)
        - normed * jnp.mean(scaled * normed, axis=-1, keepdims=True)
    )
    return (middle * inverse_dev, jnp.sum(gradients * normed, axis=0), jnp.sum(gradients, axis=0))


def swish_slope(pre_act):
    sigmoid_of = jax.nn.sigmoid(pre_act)
    return sigmoid_of * (1.0 + pre_act * (1.0 - sigmoid_of))


def block_weights(log_piece, seg_piece, seg_prior):
    cumulative = jnp.cumsum(log_piece, axis=1)
    row_index = jnp.arange(seg_piece.shape[0], dtype=jnp.int32)
    allowed = (seg_piece[:, None] == seg_piece[None, :]) & (
        row_index[:, None] >= row_index[None, :]
    )
    exponent = jnp.where(allowed[None], cumulative[:, :, None] - cumulative[:, None, :], 0.0)
    within = jnp.where(allowed[None], jnp.exp(exponent), 0.0)
    entering = jnp.where((seg_piece == seg_prior)[None, :], jnp.exp(cumulative), 0.0)
    leaving = jnp.where(
        (seg_piece == seg_piece[-1])[None, :], jnp.exp(cumulative[:, -1:] - cumulative), 0.0
    )
    return (within, entering, leaving)


def adam_step(master, first_old, second, gradient, step_rate, decay_rate):
    first_new = BETA_ONE * first_old + (1.0 - BETA_ONE) * gradient
    second_new = BETA_TWO * second + (1.0 - BETA_TWO) * gradient * gradient
    first_hat = first_new / (1.0 - BETA_ONE**STEP)
    second_hat = second_new / (1.0 - BETA_TWO**STEP)
    master_new = master - step_rate * (
        first_hat / (jnp.sqrt(second_hat) + ADAM_EPS) + decay_rate * master
    )
    return (master_new, first_new, second_new)


VEC_ROWS = 32
ROW_STEP = 256
ORDER = tuple(range(8)) + tuple(range(14, 22)) + tuple(range(8, 14))
MESH = pl.DeviceIdType.MESH


def entry_of(local_state, carry, scales):
    count = lax.axis_size("tm")
    place = lax.axis_index("tm")
    backward = scales is not None
    sent = local_state.astype(jnp.bfloat16)
    if not backward:
        row = jnp.broadcast_to(carry[:, None, None], (H, 1, P_SIZE)).astype(jnp.bfloat16)
        sent = jnp.concatenate([sent, row], axis=1)
    arrived = lax.all_gather(sent, "tm")
    if not backward:
        scales = arrived[:, :, NS, 0].astype(jnp.float32)
        arrived = arrived[:, :, :NS]
    source = jnp.arange(count)[:, None]
    between = jnp.arange(count)[None, :]
    if backward:
        passed = (between < source) & (between > place)
        ahead = source > place
    else:
        passed = (between > source) & (between < place)
        ahead = source < place
    weights = jnp.prod(jnp.where(passed[:, :, None], scales[None], 1.0), axis=1)
    weights = jnp.where(ahead, weights, 0.0)
    state = jnp.sum(weights[:, :, None, None] * arrived.astype(jnp.float32), axis=0)
    return state, scales


def halving_sum(cells, axis):
    bits = lax.axis_size(axis).bit_length() - 1
    cut = cells.shape[1] // 32 * 16
    cells = exchange_bit(cells, axis, 0, 0)
    parts = []
    for piece, order in (
        (cells[:, :cut], list(range(bits - 1))),
        (cells[:, cut:], list(reversed(range(bits - 1)))),
    ):
        left = list(range(bits - 1))
        for bit in order:
            place = left.index(bit)
            piece = exchange_bit(piece, axis, place, bit + 1)
            left.remove(bit)
        parts.append(piece[0])
    return jnp.concatenate(parts, axis=0)


def exchange_bit(cells, axis, place, bit):
    count = lax.axis_size(axis)
    mine = (lax.axis_index(axis) >> bit) & 1
    shape = cells.shape
    cells = cells.reshape(shape[0] >> (place + 1), 2, 1 << place, *shape[1:])
    kept = lax.dynamic_index_in_dim(cells, mine, 1, False)
    sent = lax.dynamic_index_in_dim(cells, 1 - mine, 1, False)
    got = lax.ppermute(sent, axis, [(i, i ^ (1 << bit)) for i in range(count)])
    total = (kept.astype(jnp.float32) + got.astype(jnp.float32)).astype(cells.dtype)
    return total.reshape(shape[0] // 2, *shape[1:])


def gather_kernel(owners, count, slots_ref, own_ref, full_ref, line, chosen, up_s, up_r, down_s, down_r, own_sem, tm_s, tm_r):
    capacity = own_ref.shape[0]
    tiles = chosen.shape[0]
    place = lax.axis_index("utt")
    me = lax.axis_index("tm")
    bits = count.bit_length() - 1
    barrier = pltpu.get_barrier_semaphore()
    for step in (1, -1):

        @pl.when((place + step >= 0) & (place + step < owners))
        def _():
            pl.semaphore_signal(
                barrier, inc=1, device_id={"utt": place + step}, device_id_type=MESH
            )

    for bit in range(bits):
        pl.semaphore_signal(
            barrier, inc=1, device_id={"tm": partner(me, 1 << bit)}, device_id_type=MESH
        )
    beside = (place + owners - 1) // owners + (2 * owners - 2 - place) // owners
    pl.semaphore_wait(barrier, bits + beside)
    own_copy = pltpu.make_async_copy(own_ref, line.at[place], own_sem.at[0])
    own_copy.start()
    own_copy.wait()

    def hop(slot, target, send, receive):
        return pltpu.make_async_remote_copy(
            src_ref=line.at[slot],
            dst_ref=line.at[slot],
            send_sem=send,
            recv_sem=receive,
            device_id={"utt": target},
            device_id_type=MESH,
        )

    def line_step(step, phase):
        lower, upper = place - step, place + step

        @pl.when((lower >= 0) & (place + 1 < owners))
        def _():
            copy = hop(lower, place + 1, up_s.at[step], up_r.at[step])
            copy.start() if phase == 0 else copy.wait_send()

        @pl.when((upper < owners) & (place >= 1))
        def _():
            copy = hop(upper, place - 1, down_s.at[step], down_r.at[step])
            copy.start() if phase == 0 else copy.wait_send()

    for step in range(owners - 1):
        line_step(step, 0)

        @pl.when(place - step >= 1)
        def _():
            hop(place - step - 1, place - 1, up_s.at[step], up_r.at[step]).wait_recv()

        @pl.when(place + step + 1 < owners)
        def _():
            hop(place + step + 1, place + 1, down_s.at[step], down_r.at[step]).wait_recv()

    for number in range(tiles):
        slot = slots_ref[ORDER[number]]
        chosen[number] = line[slot // capacity, slot % capacity]
    local = pltpu.make_async_copy(chosen, full_ref.at[me, pl.ds(0, tiles)], own_sem.at[1])
    local.start()
    local.wait()
    half = tiles // 2
    ranges = ((0, half), (half, tiles - half))
    orders = (list(range(1, bits)), list(reversed(range(1, bits))))
    used = [0, 0]
    sent = []

    def start_send(piece, offset, flip):
        start, size = ranges[piece]
        number = used[piece]
        used[piece] = number + 1
        shard = partner(me, offset)
        cells = full_ref.at[shard, pl.ds(start, size)]
        copy = pltpu.make_async_remote_copy(
            src_ref=cells,
            dst_ref=cells,
            send_sem=tm_s.at[piece, number],
            recv_sem=tm_r.at[piece, number],
            device_id={"tm": partner(me, flip)},
            device_id_type=MESH,
        )
        copy.start()
        sent.append(copy)
        return copy

    held = [[0], [0]]
    over_cores = [start_send(piece, 0, 1) for piece in range(2)]
    for level in range(bits - 1):
        moving = [
            [
                start_send(piece, offset, 1 << orders[piece][level])
                for offset in held[piece]
            ]
            for piece in range(2)
        ]
        for piece in range(2):
            flip = 1 << orders[piece][level]
            fresh = [offset ^ flip for offset in held[piece]]
            for copy, offset in zip(moving[piece], fresh):
                copy.wait_recv()
                over_cores.append(start_send(piece, offset, 1))
            held[piece] = held[piece] + fresh
    for copy in over_cores:
        copy.wait_recv()
    for copy in sent:
        copy.wait_send()
    for step in range(owners - 1):
        line_step(step, 1)


def partner(me, flip):
    for bit in range(flip.bit_length()):
        if (flip >> bit) & 1:
            me = me + (1 << bit) * (1 - 2 * ((me // (1 << bit)) % 2))
    return me


def gather_tiles(own, tile_slots):
    owners, count = lax.axis_size("utt"), lax.axis_size("tm")
    capacity, rows, width = own.shape
    tiles = tile_slots.shape[0]
    dma = pltpu.SemaphoreType.DMA
    return pl.pallas_call(
        functools.partial(gather_kernel, owners, count),
        out_shape=jax.ShapeDtypeStruct((count, 24, rows, width), own.dtype),
        in_specs=[
            pl.BlockSpec(memory_space=pltpu.SMEM),
            pl.BlockSpec(memory_space=pl.ANY),
        ],
        out_specs=pl.BlockSpec(memory_space=pl.ANY),
        scratch_shapes=[
            pltpu.VMEM((owners, capacity, rows, width), own.dtype),
            pltpu.VMEM((tiles, rows, width), own.dtype),
            dma((owners - 1,)),
            dma((owners - 1,)),
            dma((owners - 1,)),
            dma((owners - 1,)),
            dma((2,)),
            dma((2, count - 1)),
            dma((2, count - 1)),
        ],
        compiler_params=pltpu.CompilerParams(
            collective_id=0, has_side_effects=True, vmem_limit_bytes=16 << 20
        ),
    )(tile_slots, own)


def gate_of(values):
    return 0.5 * jnp.tanh(0.5 * values) + 0.5


def norm_parts(values):
    centered = values - jnp.mean(values, axis=-1, keepdims=True)
    inverse_dev = lax.rsqrt(jnp.mean(centered * centered, axis=-1, keepdims=True) + NORM_EPS)
    return centered * inverse_dev, inverse_dev


def norm_back(gradients, normed, inverse_dev, norm_gain):
    scaled = gradients * norm_gain
    middle = (
        scaled
        - jnp.mean(scaled, axis=-1, keepdims=True)
        - normed * jnp.mean(scaled * normed, axis=-1, keepdims=True)
    )
    return (
        middle * inverse_dev,
        jnp.sum(gradients * normed, axis=0, keepdims=True),
        jnp.sum(gradients, axis=0, keepdims=True),
    )


def tile_at(tiles_ref, number):
    return tiles_ref[:, number].reshape(D, D)


def first_kernel(x_ref, ffn_ref, mix_ref, vec_ref, after_ref, vals_ref, kq_ref):
    values = x_ref[...].astype(jnp.float32)
    normed, _ = norm_parts(values)
    low = (normed * vec_ref[0:1] + vec_ref[6:7]).astype(jnp.bfloat16)
    total = jnp.zeros_like(values)
    for part in range(FF // D):
        hidden = product(low, tile_at(ffn_ref, part))
        activated = (hidden * gate_of(hidden)).astype(jnp.bfloat16)
        total = total + product(activated, tile_at(ffn_ref, FF // D + part))
    after = values + 0.5 * total
    after_ref[...] = after
    normed, _ = norm_parts(after)
    low = (normed * vec_ref[1:2] + vec_ref[7:8]).astype(jnp.bfloat16)
    vals_ref[...] = product(low, tile_at(mix_ref, 0)).astype(jnp.bfloat16)
    kq_ref[...] = product(low, tile_at(mix_ref, 1)).astype(jnp.bfloat16)


def tile_block(gathered, number):
    count, _, rows, width = gathered.shape
    return pl.BlockSpec(
        (count, 8, rows, width), lambda i: (0, number, 0, 0), pipeline_mode=pl.Buffered(1)
    )


def ffn_first(inputs, gathered, vectors):
    frames = inputs.shape[0]
    rows = pl.BlockSpec((ROW_STEP, D), lambda i: (i, 0))
    return pl.pallas_call(
        first_kernel,
        grid=(frames // ROW_STEP,),
        out_shape=(
            jax.ShapeDtypeStruct((frames, D), jnp.float32),
            jax.ShapeDtypeStruct((frames, D), jnp.bfloat16),
            jax.ShapeDtypeStruct((frames, D), jnp.bfloat16),
        ),
        in_specs=[
            rows,
            tile_block(gathered, 0),
            tile_block(gathered, 2),
            pl.BlockSpec(vectors.shape, lambda i: (0, 0)),
        ],
        out_specs=(rows, rows, rows),
        compiler_params=pltpu.CompilerParams(vmem_limit_bytes=48 << 20),
    )(inputs, gathered, gathered, vectors)


def back_kernel(steps, last, norm, x_ref, grad_ref, ffn_ref, vec_ref, *refs):
    if last:
        out_ref, *refs = refs
    din_ref, tiles_ref, vsum_ref, low_s, act_s, dd_s, dh_s = refs
    step = pl.program_id(0)
    parts = FF // D

    @pl.when(step == 0)
    def _():
        vsum_ref[...] = jnp.zeros_like(vsum_ref)

    @pl.when(step < steps)
    def _():
        rows = pl.ds(pl.multiple_of(step * ROW_STEP, ROW_STEP), ROW_STEP)
        values = x_ref[...].astype(jnp.float32)
        gain, shift = vec_ref[norm : norm + 1], vec_ref[6 + norm : 7 + norm]
        normed, inverse_dev = norm_parts(values)
        low = (normed * gain + shift).astype(jnp.bfloat16)
        low_s[rows] = low
        slopes = []
        total = jnp.zeros_like(values)
        for part in range(parts):
            hidden = product(low, tile_at(ffn_ref, part))
            gate = gate_of(hidden)
            activated = (hidden * gate).astype(jnp.bfloat16)
            act_s[part, rows] = activated
            slopes.append(gate * (1.0 + hidden * (1.0 - gate)))
            if last:
                total = total + product(activated, tile_at(ffn_ref, parts + part))
        grad = grad_ref[...].astype(jnp.float32)
        if last:
            final, final_dev = norm_parts(values + 0.5 * total)
            out_ref[...] = (final * vec_ref[5:6] + vec_ref[11:12]).astype(jnp.bfloat16)
            grad, gain_sum, shift_sum = norm_back(grad, final, final_dev, vec_ref[5:6])
            vsum_ref[2:3] += gain_sum
            vsum_ref[3:4] += shift_sum
        down_in = (0.5 * grad).astype(jnp.bfloat16)
        dd_s[rows] = down_in
        total = jnp.zeros_like(values)
        for part in range(parts):
            back = input_grad(down_in, tile_at(ffn_ref, parts + part))
            hidden_grad = (back * slopes[part]).astype(jnp.bfloat16)
            dh_s[part, rows] = hidden_grad
            total = total + input_grad(hidden_grad, tile_at(ffn_ref, part))
        through, gain_sum, shift_sum = norm_back(total, normed, inverse_dev, gain)
        vsum_ref[0:1] += gain_sum
        vsum_ref[1:2] += shift_sum
        din_ref[...] = grad + through

    def put(values):
        tiles_ref[...] = values.astype(jnp.bfloat16).reshape(tiles_ref.shape)

    @pl.when((step >= steps) & (step < steps + parts))
    def _():
        put(weight_grad(low_s[...], dh_s[step - steps]))

    @pl.when(step >= steps + parts)
    def _():
        put(weight_grad(act_s[step - steps - parts], dd_s[...]))


def ffn_back_call(values, grad, gathered, vectors, own_rows, last):
    frames = values.shape[0]
    count = gathered.shape[0]
    steps = frames // ROW_STEP
    parts = FF // D
    rows = pl.BlockSpec((ROW_STEP, D), lambda i: (jnp.minimum(i, steps - 1), 0))
    out_shape = [
        jax.ShapeDtypeStruct((frames, D), jnp.float32),
        jax.ShapeDtypeStruct((count, 2 * parts, own_rows, D), jnp.bfloat16),
        jax.ShapeDtypeStruct((8, D), jnp.float32),
    ]
    out_specs = [
        rows,
        pl.BlockSpec((count, 1, own_rows, D), lambda i: (0, jnp.maximum(i - steps, 0), 0, 0)),
        pl.BlockSpec((8, D), lambda i: (0, 0)),
    ]
    if last:
        out_shape.insert(0, jax.ShapeDtypeStruct((frames, D), jnp.bfloat16))
        out_specs.insert(0, rows)
    return pl.pallas_call(
        functools.partial(back_kernel, steps, last, 4 if last else 0),
        grid=(steps + 2 * parts,),
        out_shape=out_shape,
        in_specs=[
            rows,
            rows,
            tile_block(gathered, 1 if last else 0),
            pl.BlockSpec(vectors.shape, lambda i: (0, 0)),
        ],
        out_specs=out_specs,
        scratch_shapes=[
            pltpu.VMEM((frames, D), jnp.bfloat16),
            pltpu.VMEM((parts, frames, D), jnp.bfloat16),
            pltpu.VMEM((frames, D), jnp.bfloat16),
            pltpu.VMEM((parts, frames, D), jnp.bfloat16),
        ],
        compiler_params=pltpu.CompilerParams(vmem_limit_bytes=48 << 20),
    )(values, grad, gathered, vectors)


def ffn_second(values, cotangent, gathered, vectors, own_rows):
    return ffn_back_call(values, cotangent, gathered, vectors, own_rows, True)


def ffn_back(values, grad, gathered, vectors, own_rows):
    return ffn_back_call(values, grad, gathered, vectors, own_rows, False)


def local(
    inputs,
    cotangent,
    frame_mask,
    slot_lengths,
    decays,
    tile_slots,
    master_weight_tiles,
    tile_first,
    tile_second,
    vector_master,
    vector_first,
    vector_second,
):
    own_rows, capacity, _ = master_weight_tiles.shape
    owners_count = lax.axis_size("utt")
    low_master = master_weight_tiles.transpose(1, 0, 2).astype(jnp.bfloat16)
    gathered = gather_tiles(low_master, tile_slots)
    w_values, w_states, w_output, w_linear, w_gate, w_project = [
        gathered[:, 16 + number].reshape(D, D) for number in range(6)
    ]
    norm_gains = vector_master[0:6]
    norm_shifts = vector_master[6:12]
    conv_taps = vector_master[12:]
    frames = inputs.shape[1]
    first_frame = lax.axis_index("tm") * frames
    starts = jnp.cumsum(slot_lengths[0]) - slot_lengths[0]

    def segment_of(positions):
        return jnp.sum((starts[None, :] <= positions[:, None]).astype(jnp.int32), axis=1) - 1

    positions = first_frame + jnp.arange(frames, dtype=jnp.int32)
    segments = segment_of(positions)
    seg_before = segment_of(jnp.reshape(first_frame - 1, (1,)))[0]
    log_decay = jnp.log(decays[0])
    after_a, raw_vals, key_query = ffn_first(inputs[0], gathered, vector_master)
    live_mask = frame_mask[0].astype(jnp.bfloat16)[:, None]
    state_vals = (raw_vals * live_mask).reshape(frames, H, P_SIZE)
    state_keys = key_query[:, : H * NS].reshape(frames, H, NS)
    state_query = key_query[:, H * NS :].reshape(frames, H, NS)
    keys_wide = state_keys.astype(jnp.float32)
    query_wide = state_query.astype(jnp.float32)
    vals_wide = state_vals.astype(jnp.float32)
    total_log = jnp.cumsum(log_decay, axis=1)
    tail_dev = jnp.where(
        (segments == segments[-1])[None, :], jnp.exp(total_log[:, -1:] - total_log), 0.0
    )
    local_state = jnp.einsum(
        "shn,shp->hnp", keys_wide * tail_dev.T[:, :, None], vals_wide, precision=PRECISE
    )
    carry_dev = jnp.where(segments[-1] == seg_before, jnp.exp(total_log[:, -1]), 0.0)
    entry_state, all_scales = entry_of(local_state, carry_dev, None)
    count_blocks = frames // BLK
    saved_blocks = []
    outputs = []
    run_state = entry_state
    for number in range(count_blocks):
        block_start = number * BLK
        rows_here = slice(block_start, block_start + BLK)
        if number == 0:
            seg_prior = seg_before
        else:
            seg_prior = segments[block_start - 1]
        within, entering, leaving = block_weights(
            log_decay[:, rows_here], segments[rows_here], seg_prior
        )
        scores = jnp.einsum(
            "thn,shn->hts",
            state_query[rows_here],
            state_keys[rows_here],
            preferred_element_type=jnp.float32,
        )
        mixed_low = (within * scores).astype(jnp.bfloat16)
        inner_part = jnp.einsum(
            "hts,shp->thp", mixed_low, state_vals[rows_here], preferred_element_type=jnp.float32
        )
        carried = jnp.einsum(
            "thn,hnp->thp",
            query_wide[rows_here] * entering.T[:, :, None],
            run_state,
            precision=PRECISE,
        )
        outputs.append(inner_part + carried)
        saved_blocks.append((within, entering, leaving, mixed_low, run_state))
        run_state = (
            jnp.einsum(
                "shn,shp->hnp",
                keys_wide[rows_here] * leaving.T[:, :, None],
                vals_wide[rows_here],
                precision=PRECISE,
            )
            + entering[:, -1][:, None, None] * run_state
        )
    low_y = jnp.concatenate(outputs, axis=0).reshape(frames, H * P_SIZE).astype(jnp.bfloat16)
    after_b = after_a + product(low_y, w_output)
    normed_c_out, unit_c, inverse_c = layer_norm(after_b, norm_gains[2], norm_shifts[2])
    low_c = normed_c_out.astype(jnp.bfloat16)
    part_lin = product(low_c, w_linear)
    part_gate = product(low_c, w_gate)
    gate_sigmoid = jax.nn.sigmoid(part_gate)
    glu_low = (part_lin * gate_sigmoid).astype(jnp.bfloat16)
    half_width = K // 2
    padded = padded_2(glu_low, (("tm", 0),), half_width)
    pad_positions = first_frame - half_width + jnp.arange(frames + 2 * half_width, dtype=jnp.int32)
    pad_segments = segment_of(pad_positions)
    tap_masks = [
        (pad_segments[kernel_offset : kernel_offset + frames] == segments).astype(jnp.float32)[
            :, None
        ]
        for kernel_offset in range(K)
    ]
    conv_sum = jnp.zeros((frames, D), jnp.float32)
    for kernel_offset in range(K):
        conv_sum = (
            conv_sum
            + conv_taps[kernel_offset]
            * padded[kernel_offset : kernel_offset + frames].astype(jnp.float32)
            * tap_masks[kernel_offset]
        )
    normed_d, unit_d, inverse_d = layer_norm(conv_sum, norm_gains[3], norm_shifts[3])
    low_d = (normed_d * jax.nn.sigmoid(normed_d)).astype(jnp.bfloat16)
    after_c = after_b + product(low_d, w_project)
    output, grad_c, tile_grads_e, vec_e = ffn_second(
        after_c, cotangent[0], gathered, vector_master, own_rows
    )
    output = output[None]
    gain_e, shift_e, gain_f, shift_f = vec_e[0], vec_e[1], vec_e[2], vec_e[3]
    project_in = grad_c.astype(jnp.bfloat16)
    grad_project = weight_grad(low_d, project_in)
    grad_swish = input_grad(project_in, w_project) * swish_slope(normed_d)
    grad_conv, gain_d, shift_d = norm_grad(grad_swish, unit_d, inverse_d, norm_gains[3])
    low_grad_conv = grad_conv.astype(jnp.bfloat16)
    grad_padded = padded_2(low_grad_conv, (("tm", 0),), half_width)
    grad_conv_wide = low_grad_conv.astype(jnp.float32)
    grad_glu = jnp.zeros((frames, D), jnp.float32)
    tap_grads = []
    for kernel_offset in range(K):
        back_start = 2 * half_width - kernel_offset
        grad_glu = (
            grad_glu
            + conv_taps[kernel_offset]
            * grad_padded[back_start : back_start + frames].astype(jnp.float32)
            * tap_masks[K - 1 - kernel_offset]
        )
        tap_grads.append(
            jnp.sum(
                grad_conv_wide
                * padded[kernel_offset : kernel_offset + frames].astype(jnp.float32)
                * tap_masks[kernel_offset],
                axis=0,
            )
        )
    grad_lin = (grad_glu * gate_sigmoid).astype(jnp.bfloat16)
    grad_gate = (grad_glu * part_lin * gate_sigmoid * (1.0 - gate_sigmoid)).astype(jnp.bfloat16)
    grad_w_linear = weight_grad(low_c, grad_lin)
    grad_w_gate = weight_grad(low_c, grad_gate)
    grad_in_c, gain_c, shift_c = norm_grad(
        input_grad(grad_lin, w_linear) + input_grad(grad_gate, w_gate),
        unit_c,
        inverse_c,
        norm_gains[2],
    )
    grad_b = grad_c + grad_in_c
    output_in = grad_b.astype(jnp.bfloat16)
    grad_w_output = weight_grad(low_y, output_in)
    grad_y = input_grad(output_in, w_output).astype(jnp.bfloat16).reshape(frames, H, P_SIZE)
    grad_y_wide = grad_y.astype(jnp.float32)
    entering_dev = jnp.where((segments == seg_before)[None, :], jnp.exp(total_log), 0.0)
    local_back = jnp.einsum(
        "thn,thp->hnp", query_wide * entering_dev.T[:, :, None], grad_y_wide, precision=PRECISE
    )
    exit_grad, _ = entry_of(local_back, carry_dev, all_scales)
    incoming = exit_grad
    vals_parts = []
    keys_parts = []
    query_parts = []
    for number in reversed(range(count_blocks)):
        block_start = number * BLK
        rows_here = slice(block_start, block_start + BLK)
        within, entering, leaving, mixed_low, prior_state = saved_blocks[number]
        grad_blk = grad_y[rows_here]
        grad_blk_wide = grad_y_wide[rows_here]
        grad_mixed = jnp.einsum(
            "thp,shp->hts", grad_blk, state_vals[rows_here], preferred_element_type=jnp.float32
        )
        grad_vals = jnp.einsum(
            "hts,thp->shp", mixed_low, grad_blk, preferred_element_type=jnp.float32
        )
        grad_scores = (within * grad_mixed).astype(jnp.bfloat16)
        grad_query = jnp.einsum(
            "hts,shn->thn", grad_scores, state_keys[rows_here], preferred_element_type=jnp.float32
        )
        grad_keys = jnp.einsum(
            "hts,thn->shn", grad_scores, state_query[rows_here], preferred_element_type=jnp.float32
        )
        grad_query = grad_query + entering.T[:, :, None] * jnp.einsum(
            "thp,hnp->thn", grad_blk_wide, prior_state, precision=PRECISE
        )
        grad_vals = grad_vals + jnp.einsum(
            "shn,hnp->shp",
            keys_wide[rows_here] * leaving.T[:, :, None],
            incoming,
            precision=PRECISE,
        )
        grad_keys = grad_keys + leaving.T[:, :, None] * jnp.einsum(
            "shp,hnp->shn", vals_wide[rows_here], incoming, precision=PRECISE
        )
        incoming = (
            jnp.einsum(
                "thn,thp->hnp",
                query_wide[rows_here] * entering.T[:, :, None],
                grad_blk_wide,
                precision=PRECISE,
            )
            + entering[:, -1][:, None, None] * incoming
        )
        vals_parts.insert(0, grad_vals)
        keys_parts.insert(0, grad_keys)
        query_parts.insert(0, grad_query)
    grad_v_low = (
        jnp.concatenate(vals_parts, axis=0).reshape(frames, D) * live_mask.astype(jnp.float32)
    ).astype(jnp.bfloat16)
    grad_kq_low = jnp.concatenate(
        [
            jnp.concatenate(keys_parts, axis=0).reshape(frames, H * NS),
            jnp.concatenate(query_parts, axis=0).reshape(frames, H * NS),
        ],
        axis=1,
    ).astype(jnp.bfloat16)
    low_b = layer_norm(after_a, norm_gains[1], norm_shifts[1])[0].astype(jnp.bfloat16)
    grad_w_values = weight_grad(low_b, grad_v_low)
    grad_w_states = weight_grad(low_b, grad_kq_low)
    _, unit_b, inverse_b = layer_norm(after_a, norm_gains[1], norm_shifts[1])
    grad_in_b, gain_b, shift_b = norm_grad(
        input_grad(grad_v_low, w_values) + input_grad(grad_kq_low, w_states),
        unit_b,
        inverse_b,
        norm_gains[1],
    )
    grad_a = grad_b + grad_in_b
    grad_start, tile_grads_a, vec_a = ffn_back(
        inputs[0], grad_a, gathered, vector_master, own_rows
    )
    gain_a, shift_a = vec_a[0], vec_a[1]
    count = lax.axis_size("tm")
    vector_grad = jnp.concatenate(
        [
            jnp.stack(
                [
                    gain_a,
                    gain_b,
                    gain_c,
                    gain_d,
                    gain_e,
                    gain_f,
                    shift_a,
                    shift_b,
                    shift_c,
                    shift_d,
                    shift_e,
                    shift_f,
                ]
            ),
            jnp.stack(tap_grads),
        ],
        axis=0,
    )
    mixers = jnp.stack(
        [grad_w_values, grad_w_states, grad_w_output, grad_w_linear, grad_w_gate, grad_project]
    ).astype(jnp.bfloat16)
    mixers = mixers.reshape(6, count, own_rows, D).transpose(1, 0, 2, 3)
    tail = jnp.zeros((VEC_ROWS - vector_grad.shape[0], D), jnp.float32)
    vectors = jnp.concatenate([vector_grad, tail], axis=0).astype(jnp.bfloat16)
    shards_e = halving_sum(tile_grads_e.reshape(count, 8 * own_rows, D), "tm")
    shards_m = halving_sum(mixers.reshape(count, 6 * own_rows, D), "tm")
    shards_a = halving_sum(
        jnp.concatenate(
            [
                tile_grads_a.reshape(count, 8 * own_rows, D),
                jnp.broadcast_to(vectors[None], (count, VEC_ROWS, D)),
            ],
            axis=1,
        ),
        "tm",
    )
    shards = jnp.concatenate(
        [
            shards_a[: 8 * own_rows].reshape(8, own_rows, D),
            shards_m.reshape(6, own_rows, D),
            shards_e.reshape(8, own_rows, D),
            jnp.zeros((1, own_rows, D), jnp.bfloat16),
        ],
        axis=0,
    )
    tiles = tile_slots.shape[0]
    tile_of = (
        jnp.full((owners_count * capacity,), tiles, jnp.int32)
        .at[tile_slots]
        .set(jnp.arange(tiles, dtype=jnp.int32))
    )
    placed = shards[tile_of].reshape(owners_count, capacity * own_rows, D)
    shared = jnp.broadcast_to(shards_a[None, 8 * own_rows :], (owners_count, VEC_ROWS, D))
    reduced = lax.psum_scatter(
        jnp.concatenate([placed, shared], axis=1), "utt", scatter_dimension=0
    ).astype(jnp.float32)
    vector_total = reduced[capacity * own_rows :][: vector_grad.shape[0]]
    reduced = reduced[: capacity * own_rows].reshape(capacity, own_rows, D).transpose(1, 0, 2)
    tile_new, first_new, second_new = adam_step(
        master_weight_tiles, tile_first, tile_second, reduced, RATE_TILES, DECAY_TILES
    )
    vector_new, vfirst_new, vsecond_new = adam_step(
        vector_master, vector_first, vector_second, vector_total, RATE_VECTORS, 0.0
    )
    return (
        output,
        grad_start[None],
        tile_new,
        first_new,
        second_new,
        tile_new.astype(jnp.bfloat16),
        vector_new,
        vfirst_new,
        vsecond_new,
    )


def solution(mesh):
    in_specs = (
        P("utt", "tm", None),
        P("utt", "tm", None),
        P("utt", "tm"),
        P("utt", None),
        P("utt", None, "tm"),
        P(),
        P(("utt", "tm"), None, None),
        P(("utt", "tm"), None, None),
        P(("utt", "tm"), None, None),
        P(),
        P(),
        P(),
    )
    out_specs = (
        P("utt", "tm", None),
        P("utt", "tm", None),
        P(("utt", "tm"), None, None),
        P(("utt", "tm"), None, None),
        P(("utt", "tm"), None, None),
        P(("utt", "tm"), None, None),
        P(),
        P(),
        P(),
    )
    return jax.shard_map(local, mesh=mesh, in_specs=in_specs, out_specs=out_specs, check_vma=False)
```

```python
import functools

import jax
import jax.numpy as jnp
from jax import lax
from jax.experimental import pallas as pl
from jax.experimental.pallas import tpu as pltpu
from jax.sharding import PartitionSpec as P

D = 512
FF = 2048
H = 8
NS = 32
K = 15
BLK = 512
STEP = 7
P_SIZE = 64


NORM_EPS = 1e-05
ADAM_EPS = 1e-08
BETA_ONE = 0.9
BETA_TWO = 0.999
RATE_TILES = 0.04
RATE_VECTORS = 0.1
DECAY_TILES = 0.1
PRECISE = lax.Precision.HIGHEST


def padded_2(cells, sides, width):
    for axis, dim in sides:
        count = lax.axis_size(axis)
        ends = count - 1
        head = lax.slice_in_dim(cells, 0, width, axis=dim)
        tail = lax.slice_in_dim(cells, cells.shape[dim] - width, cells.shape[dim], axis=dim)
        cells = jnp.concatenate(
            [
                lax.ppermute(tail, axis, [(i, (i + 1) % count) for i in range(ends)]),
                cells,
                lax.ppermute(head, axis, [((i + 1) % count, i) for i in range(ends)]),
            ],
            axis=dim,
        )
    return cells


def product(matrix_a, matrix_b):
    return jnp.dot(matrix_a, matrix_b, preferred_element_type=jnp.float32)


def weight_grad(activations, gradients):
    return lax.dot_general(
        activations, gradients, (((0,), (0,)), ((), ())), preferred_element_type=jnp.float32
    )


def input_grad(gradients, weights):
    return lax.dot_general(
        gradients, weights, (((1,), (1,)), ((), ())), preferred_element_type=jnp.float32
    )


def layer_norm(values, norm_gain, norm_shift):
    centered = values - jnp.mean(values, axis=-1, keepdims=True)
    inverse_dev = lax.rsqrt(jnp.mean(centered * centered, axis=-1, keepdims=True) + NORM_EPS)
    normed = centered * inverse_dev
    return (normed * norm_gain + norm_shift, normed, inverse_dev)


def norm_grad(gradients, normed, inverse_dev, norm_gain):
    scaled = gradients * norm_gain
    middle = (
        scaled
        - jnp.mean(scaled, axis=-1, keepdims=True)
        - normed * jnp.mean(scaled * normed, axis=-1, keepdims=True)
    )
    return (middle * inverse_dev, jnp.sum(gradients * normed, axis=0), jnp.sum(gradients, axis=0))


def swish_slope(pre_act):
    sigmoid_of = jax.nn.sigmoid(pre_act)
    return sigmoid_of * (1.0 + pre_act * (1.0 - sigmoid_of))


def adam_step(master, first_old, second, gradient, step_rate, decay_rate):
    first_new = BETA_ONE * first_old + (1.0 - BETA_ONE) * gradient
    second_new = BETA_TWO * second + (1.0 - BETA_TWO) * gradient * gradient
    first_hat = first_new / (1.0 - BETA_ONE**STEP)
    second_hat = second_new / (1.0 - BETA_TWO**STEP)
    master_new = master - step_rate * (
        first_hat / (jnp.sqrt(second_hat) + ADAM_EPS) + decay_rate * master
    )
    return (master_new, first_new, second_new)


VEC_ROWS = 32
ROW_STEP = 256
ORDER = tuple(range(8)) + tuple(range(14, 22)) + tuple(range(8, 14))
MESH = pl.DeviceIdType.MESH


def halving_sum(cells, axis):
    bits = lax.axis_size(axis).bit_length() - 1
    cut = cells.shape[1] // 32 * 16
    cells = exchange_bit(cells, axis, 0, 0)
    parts = []
    for piece, order in (
        (cells[:, :cut], list(range(bits - 1))),
        (cells[:, cut:], list(reversed(range(bits - 1)))),
    ):
        left = list(range(bits - 1))
        for bit in order:
            place = left.index(bit)
            piece = exchange_bit(piece, axis, place, bit + 1)
            left.remove(bit)
        parts.append(piece[0])
    return jnp.concatenate(parts, axis=0)


def exchange_bit(cells, axis, place, bit):
    count = lax.axis_size(axis)
    mine = (lax.axis_index(axis) >> bit) & 1
    shape = cells.shape
    cells = cells.reshape(shape[0] >> (place + 1), 2, 1 << place, *shape[1:])
    kept = lax.dynamic_index_in_dim(cells, mine, 1, False)
    sent = lax.dynamic_index_in_dim(cells, 1 - mine, 1, False)
    got = lax.ppermute(sent, axis, [(i, i ^ (1 << bit)) for i in range(count)])
    total = (kept.astype(jnp.float32) + got.astype(jnp.float32)).astype(cells.dtype)
    return total.reshape(shape[0] // 2, *shape[1:])


def gather_kernel(owners, count, slots_ref, own_ref, full_ref, line, chosen, up_s, up_r, down_s, down_r, own_sem, tm_s, tm_r):
    capacity = own_ref.shape[0]
    tiles = chosen.shape[0]
    place = lax.axis_index("utt")
    me = lax.axis_index("tm")
    bits = count.bit_length() - 1
    barrier = pltpu.get_barrier_semaphore()
    for step in (1, -1):

        @pl.when((place + step >= 0) & (place + step < owners))
        def _():
            pl.semaphore_signal(
                barrier, inc=1, device_id={"utt": place + step}, device_id_type=MESH
            )

    for bit in range(bits):
        pl.semaphore_signal(
            barrier, inc=1, device_id={"tm": partner(me, 1 << bit)}, device_id_type=MESH
        )
    beside = (place + owners - 1) // owners + (2 * owners - 2 - place) // owners
    pl.semaphore_wait(barrier, bits + beside)
    own_copy = pltpu.make_async_copy(own_ref, line.at[place], own_sem.at[0])
    own_copy.start()
    own_copy.wait()

    def hop(slot, target, send, receive):
        return pltpu.make_async_remote_copy(
            src_ref=line.at[slot],
            dst_ref=line.at[slot],
            send_sem=send,
            recv_sem=receive,
            device_id={"utt": target},
            device_id_type=MESH,
        )

    def line_step(step, phase):
        lower, upper = place - step, place + step

        @pl.when((lower >= 0) & (place + 1 < owners))
        def _():
            copy = hop(lower, place + 1, up_s.at[step], up_r.at[step])
            copy.start() if phase == 0 else copy.wait_send()

        @pl.when((upper < owners) & (place >= 1))
        def _():
            copy = hop(upper, place - 1, down_s.at[step], down_r.at[step])
            copy.start() if phase == 0 else copy.wait_send()

    for step in range(owners - 1):
        line_step(step, 0)

        @pl.when(place - step >= 1)
        def _():
            hop(place - step - 1, place - 1, up_s.at[step], up_r.at[step]).wait_recv()

        @pl.when(place + step + 1 < owners)
        def _():
            hop(place + step + 1, place + 1, down_s.at[step], down_r.at[step]).wait_recv()

    for number in range(tiles):
        slot = slots_ref[ORDER[number]]
        chosen[number] = line[slot // capacity, slot % capacity]
    local = pltpu.make_async_copy(chosen, full_ref.at[me, pl.ds(0, tiles)], own_sem.at[1])
    local.start()
    local.wait()
    half = tiles // 2
    ranges = ((0, half), (half, tiles - half))
    orders = (list(range(1, bits)), list(reversed(range(1, bits))))
    used = [0, 0]
    sent = []

    def start_send(piece, offset, flip):
        start, size = ranges[piece]
        number = used[piece]
        used[piece] = number + 1
        shard = partner(me, offset)
        cells = full_ref.at[shard, pl.ds(start, size)]
        copy = pltpu.make_async_remote_copy(
            src_ref=cells,
            dst_ref=cells,
            send_sem=tm_s.at[piece, number],
            recv_sem=tm_r.at[piece, number],
            device_id={"tm": partner(me, flip)},
            device_id_type=MESH,
        )
        copy.start()
        sent.append(copy)
        return copy

    held = [[0], [0]]
    over_cores = [start_send(piece, 0, 1) for piece in range(2)]
    for level in range(bits - 1):
        moving = [
            [
                start_send(piece, offset, 1 << orders[piece][level])
                for offset in held[piece]
            ]
            for piece in range(2)
        ]
        for piece in range(2):
            flip = 1 << orders[piece][level]
            fresh = [offset ^ flip for offset in held[piece]]
            for copy, offset in zip(moving[piece], fresh):
                copy.wait_recv()
                over_cores.append(start_send(piece, offset, 1))
            held[piece] = held[piece] + fresh
    for copy in over_cores:
        copy.wait_recv()
    for copy in sent:
        copy.wait_send()
    for step in range(owners - 1):
        line_step(step, 1)


def partner(me, flip):
    for bit in range(flip.bit_length()):
        if (flip >> bit) & 1:
            me = me + (1 << bit) * (1 - 2 * ((me // (1 << bit)) % 2))
    return me


def gather_tiles(own, tile_slots):
    owners, count = lax.axis_size("utt"), lax.axis_size("tm")
    capacity, rows, width = own.shape
    tiles = tile_slots.shape[0]
    dma = pltpu.SemaphoreType.DMA
    return pl.pallas_call(
        functools.partial(gather_kernel, owners, count),
        out_shape=jax.ShapeDtypeStruct((count, 24, rows, width), own.dtype),
        in_specs=[
            pl.BlockSpec(memory_space=pltpu.SMEM),
            pl.BlockSpec(memory_space=pl.ANY),
        ],
        out_specs=pl.BlockSpec(memory_space=pl.ANY),
        scratch_shapes=[
            pltpu.VMEM((owners, capacity, rows, width), own.dtype),
            pltpu.VMEM((tiles, rows, width), own.dtype),
            dma((owners - 1,)),
            dma((owners - 1,)),
            dma((owners - 1,)),
            dma((owners - 1,)),
            dma((2,)),
            dma((2, count - 1)),
            dma((2, count - 1)),
        ],
        compiler_params=pltpu.CompilerParams(
            collective_id=0, has_side_effects=True, vmem_limit_bytes=16 << 20
        ),
    )(tile_slots, own)


def gate_of(values):
    return 0.5 * jnp.tanh(0.5 * values) + 0.5


def norm_parts(values):
    centered = values - jnp.mean(values, axis=-1, keepdims=True)
    inverse_dev = lax.rsqrt(jnp.mean(centered * centered, axis=-1, keepdims=True) + NORM_EPS)
    return centered * inverse_dev, inverse_dev


def norm_back(gradients, normed, inverse_dev, norm_gain):
    scaled = gradients * norm_gain
    middle = (
        scaled
        - jnp.mean(scaled, axis=-1, keepdims=True)
        - normed * jnp.mean(scaled * normed, axis=-1, keepdims=True)
    )
    return (
        middle * inverse_dev,
        jnp.sum(gradients * normed, axis=0, keepdims=True),
        jnp.sum(gradients, axis=0, keepdims=True),
    )


def tile_at(tiles_ref, number):
    return tiles_ref[:, number].reshape(D, D)


def first_kernel(x_ref, ffn_ref, mix_ref, vec_ref, after_ref, vals_ref, kq_ref):
    values = x_ref[...].astype(jnp.float32)
    normed, _ = norm_parts(values)
    low = (normed * vec_ref[0:1] + vec_ref[6:7]).astype(jnp.bfloat16)
    total = jnp.zeros_like(values)
    for part in range(FF // D):
        hidden = product(low, tile_at(ffn_ref, part))
        activated = (hidden * gate_of(hidden)).astype(jnp.bfloat16)
        total = total + product(activated, tile_at(ffn_ref, FF // D + part))
    after = values + 0.5 * total
    after_ref[...] = after
    normed, _ = norm_parts(after)
    low = (normed * vec_ref[1:2] + vec_ref[7:8]).astype(jnp.bfloat16)
    vals_ref[...] = product(low, tile_at(mix_ref, 0)).astype(jnp.bfloat16)
    kq_ref[...] = product(low, tile_at(mix_ref, 1)).astype(jnp.bfloat16)


def tile_block(gathered, number):
    count, _, rows, width = gathered.shape
    return pl.BlockSpec(
        (count, 8, rows, width), lambda i: (0, number, 0, 0), pipeline_mode=pl.Buffered(1)
    )


def ffn_first(inputs, gathered, vectors):
    frames = inputs.shape[0]
    rows = pl.BlockSpec((ROW_STEP, D), lambda i: (i, 0))
    return pl.pallas_call(
        first_kernel,
        grid=(frames // ROW_STEP,),
        out_shape=(
            jax.ShapeDtypeStruct((frames, D), jnp.float32),
            jax.ShapeDtypeStruct((frames, D), jnp.bfloat16),
            jax.ShapeDtypeStruct((frames, D), jnp.bfloat16),
        ),
        in_specs=[
            rows,
            tile_block(gathered, 0),
            tile_block(gathered, 2),
            pl.BlockSpec(vectors.shape, lambda i: (0, 0)),
        ],
        out_specs=(rows, rows, rows),
        compiler_params=pltpu.CompilerParams(vmem_limit_bytes=48 << 20),
    )(inputs, gathered, gathered, vectors)


def back_kernel(steps, last, norm, x_ref, grad_ref, ffn_ref, vec_ref, *refs):
    if last:
        out_ref, *refs = refs
    din_ref, tiles_ref, vsum_ref, low_s, act_s, dd_s, dh_s = refs
    step = pl.program_id(0)
    parts = FF // D

    @pl.when(step == 0)
    def _():
        vsum_ref[...] = jnp.zeros_like(vsum_ref)

    @pl.when(step < steps)
    def _():
        rows = pl.ds(pl.multiple_of(step * ROW_STEP, ROW_STEP), ROW_STEP)
        values = x_ref[...].astype(jnp.float32)
        gain, shift = vec_ref[norm : norm + 1], vec_ref[6 + norm : 7 + norm]
        normed, inverse_dev = norm_parts(values)
        low = (normed * gain + shift).astype(jnp.bfloat16)
        low_s[rows] = low
        slopes = []
        total = jnp.zeros_like(values)
        for part in range(parts):
            hidden = product(low, tile_at(ffn_ref, part))
            gate = gate_of(hidden)
            activated = (hidden * gate).astype(jnp.bfloat16)
            act_s[part, rows] = activated
            slopes.append(gate * (1.0 + hidden * (1.0 - gate)))
            if last:
                total = total + product(activated, tile_at(ffn_ref, parts + part))
        grad = grad_ref[...].astype(jnp.float32)
        if last:
            final, final_dev = norm_parts(values + 0.5 * total)
            out_ref[...] = (final * vec_ref[5:6] + vec_ref[11:12]).astype(jnp.bfloat16)
            grad, gain_sum, shift_sum = norm_back(grad, final, final_dev, vec_ref[5:6])
            vsum_ref[2:3] += gain_sum
            vsum_ref[3:4] += shift_sum
        down_in = (0.5 * grad).astype(jnp.bfloat16)
        dd_s[rows] = down_in
        total = jnp.zeros_like(values)
        for part in range(parts):
            back = input_grad(down_in, tile_at(ffn_ref, parts + part))
            hidden_grad = (back * slopes[part]).astype(jnp.bfloat16)
            dh_s[part, rows] = hidden_grad
            total = total + input_grad(hidden_grad, tile_at(ffn_ref, part))
        through, gain_sum, shift_sum = norm_back(total, normed, inverse_dev, gain)
        vsum_ref[0:1] += gain_sum
        vsum_ref[1:2] += shift_sum
        din_ref[...] = grad + through

    def put(values):
        tiles_ref[...] = values.astype(jnp.bfloat16).reshape(tiles_ref.shape)

    @pl.when((step >= steps) & (step < steps + parts))
    def _():
        put(weight_grad(low_s[...], dh_s[step - steps]))

    @pl.when(step >= steps + parts)
    def _():
        put(weight_grad(act_s[step - steps - parts], dd_s[...]))


def ffn_back_call(values, grad, gathered, vectors, own_rows, last):
    frames = values.shape[0]
    count = gathered.shape[0]
    steps = frames // ROW_STEP
    parts = FF // D
    rows = pl.BlockSpec((ROW_STEP, D), lambda i: (jnp.minimum(i, steps - 1), 0))
    out_shape = [
        jax.ShapeDtypeStruct((frames, D), jnp.float32),
        jax.ShapeDtypeStruct((count, 2 * parts, own_rows, D), jnp.bfloat16),
        jax.ShapeDtypeStruct((8, D), jnp.float32),
    ]
    out_specs = [
        rows,
        pl.BlockSpec((count, 1, own_rows, D), lambda i: (0, jnp.maximum(i - steps, 0), 0, 0)),
        pl.BlockSpec((8, D), lambda i: (0, 0)),
    ]
    if last:
        out_shape.insert(0, jax.ShapeDtypeStruct((frames, D), jnp.bfloat16))
        out_specs.insert(0, rows)
    return pl.pallas_call(
        functools.partial(back_kernel, steps, last, 4 if last else 0),
        grid=(steps + 2 * parts,),
        out_shape=out_shape,
        in_specs=[
            rows,
            rows,
            tile_block(gathered, 1 if last else 0),
            pl.BlockSpec(vectors.shape, lambda i: (0, 0)),
        ],
        out_specs=out_specs,
        scratch_shapes=[
            pltpu.VMEM((frames, D), jnp.bfloat16),
            pltpu.VMEM((parts, frames, D), jnp.bfloat16),
            pltpu.VMEM((frames, D), jnp.bfloat16),
            pltpu.VMEM((parts, frames, D), jnp.bfloat16),
        ],
        compiler_params=pltpu.CompilerParams(vmem_limit_bytes=48 << 20),
    )(values, grad, gathered, vectors)


def ffn_second(values, cotangent, gathered, vectors, own_rows):
    return ffn_back_call(values, cotangent, gathered, vectors, own_rows, True)


def ffn_back(values, grad, gathered, vectors, own_rows):
    return ffn_back_call(values, grad, gathered, vectors, own_rows, False)


def scan_lanes(values):
    lane = lax.broadcasted_iota(jnp.int32, values.shape, 1)
    shift = 1
    while shift < values.shape[1]:
        values = values + jnp.where(lane >= shift, pltpu.roll(values, shift, 1), 0.0)
        shift *= 2
    return values


def segment_in(starts_ref, positions):
    found = jnp.full_like(positions, -1)
    for number in range(starts_ref.shape[0] - 1):
        found = found + (starts_ref[number] <= positions).astype(jnp.int32)
    return found


def segment_at(starts_ref, position):
    found = jnp.int32(-1)
    for number in range(starts_ref.shape[0] - 1):
        found = found + jnp.where(starts_ref[number] <= position, 1, 0)
    return found


def block_parts(starts_ref, decay_ref, block):
    base = starts_ref[starts_ref.shape[0] - 1] + block * BLK
    cumulative = scan_lanes(jnp.log(decay_ref[...]))
    row = segment_in(starts_ref, base + lax.broadcasted_iota(jnp.int32, (1, BLK), 1))
    prior = segment_at(starts_ref, base - 1)
    final = segment_at(starts_ref, base + BLK - 1)
    entering = jnp.where(row == prior, jnp.exp(cumulative), 0.0)
    leaving = jnp.where(row == final, jnp.exp(cumulative[:, BLK - 1 :] - cumulative), 0.0)
    return base, cumulative, row, entering, leaving


def per_lane(values, width):
    shape = (H, H * width)
    chosen = lax.broadcasted_iota(jnp.int32, shape, 0) == (
        lax.broadcasted_iota(jnp.int32, shape, 1) // width
    )
    return weight_grad(values.astype(jnp.bfloat16), chosen.astype(jnp.bfloat16))


def own_heads(values):
    shape = (H * NS, H * P_SIZE)
    same = (lax.broadcasted_iota(jnp.int32, shape, 0) // NS) == (
        lax.broadcasted_iota(jnp.int32, shape, 1) // P_SIZE
    )
    return jnp.where(same, values, 0.0)


def pack_state(state):
    folded = state[:, 0:128] + state[:, 128:256] + state[:, 256:384] + state[:, 384:512]
    folded = folded + pltpu.roll(folded, 64, 1)
    lane = lax.broadcasted_iota(jnp.int32, (128, 128), 1)
    return jnp.where(lane < 64, folded[0:128], folded[128:256])


def unpack_state(packed):
    turned = pltpu.roll(packed, 64, 1)
    lane = lax.broadcasted_iota(jnp.int32, (128, 128), 1)
    both = jnp.concatenate(
        [jnp.where(lane < 64, packed, turned), jnp.where(lane < 64, turned, packed)], axis=0
    )
    return own_heads(jnp.concatenate([both] * 4, axis=1))


def lanes_of(values, head, width):
    first = head * width // 128 * 128
    whole = values[:, first : first + 128]
    lane = lax.broadcasted_iota(jnp.int32, whole.shape, 1) + first
    return whole, jnp.where(lane // width == head, whole, jnp.zeros_like(whole))


def fill_bias(starts_ref, bias_s, base, row):
    column = segment_in(starts_ref, base + lax.broadcasted_iota(jnp.int32, (BLK, 1), 0))
    shape = (BLK, BLK)
    later = lax.broadcasted_iota(jnp.int32, shape, 0) >= lax.broadcasted_iota(jnp.int32, shape, 1)
    bias_s[...] = jnp.where((column == row) & later, 0.0, -1e30)


def advance(keys, values, weights, state):
    spread = per_lane(weights[0], P_SIZE)
    added = weight_grad(keys, (values.astype(jnp.float32) * spread).astype(jnp.bfloat16))
    return own_heads(added) + weights[1] * state


def summary_kernel(backward, starts_ref, decay_ref, kq_ref, vals_ref, out_ref, state_s, carry_s):
    step = pl.program_id(0)
    blocks = pl.num_programs(0)

    @pl.when(step == 0)
    def _():
        state_s[...] = jnp.zeros_like(state_s)
        carry_s[...] = jnp.ones_like(carry_s)

    block = blocks - 1 - step if backward else step
    _, _, _, entering, leaving = block_parts(starts_ref, decay_ref, block)
    spread_last = per_lane(entering, P_SIZE)[BLK - 1 :]
    if backward:
        keys, weights = kq_ref[:, H * NS :], entering
    else:
        keys, weights = kq_ref[:, : H * NS], leaving
    state_s[...] = advance(keys, vals_ref[...], (weights, spread_last), state_s[...])
    carry_s[...] = carry_s[...] * entering[:, BLK - 1 :]

    @pl.when(step == blocks - 1)
    def _():
        rest = jnp.concatenate([carry_s[...], jnp.zeros_like(carry_s)], axis=0)
        out_ref[...] = jnp.concatenate([pack_state(state_s[...]), rest], axis=0).astype(
            jnp.bfloat16
        )


def mixing_kernel(starts_ref, decay_ref, kq_ref, vals_ref, entry_ref, y_ref, saved_ref, state_s, bias_s):
    step = pl.program_id(0)

    @pl.when(step == 0)
    def _():
        state_s[...] = unpack_state(entry_ref[...])

    base, cumulative, row, entering, leaving = block_parts(starts_ref, decay_ref, step)
    fill_bias(starts_ref, bias_s, base, row)
    columns = cumulative.T
    keys, queries, values = kq_ref[:, : H * NS], kq_ref[:, H * NS :], vals_ref[...]
    spread = per_lane(entering, P_SIZE)
    low_state = state_s[...].astype(jnp.bfloat16)
    saved_ref[0] = low_state
    carried = product(queries, low_state) * spread
    half = BLK // 2
    for pair in range(H // 2):
        sums = [carried[:half, pair * 128 : pair * 128 + 128], carried[half:, pair * 128 : pair * 128 + 128]]
        for head in (2 * pair, 2 * pair + 1):
            _, query = lanes_of(queries, head, NS)
            key, _ = lanes_of(keys, head, NS)
            _, value = lanes_of(values, head, P_SIZE)
            for part in range(2):
                rows = slice(part * half, part * half + half)
                seen = (part + 1) * half
                scores = input_grad(query[rows], key[:seen])
                within = jnp.exp(
                    columns[rows, head : head + 1]
                    - cumulative[head : head + 1, :seen]
                    + bias_s[rows, :seen]
                )
                mixed = (within * scores).astype(jnp.bfloat16)
                sums[part] = sums[part] + product(mixed, value[:seen])
        for part in range(2):
            y_ref[part * half : part * half + half, pair * 128 : pair * 128 + 128] = sums[
                part
            ].astype(jnp.bfloat16)
    state_s[...] = advance(keys, values, (leaving, spread[BLK - 1 :]), state_s[...])


def unmixing_kernel(
    starts_ref, decay_ref, kq_ref, vals_ref, dy_ref, saved_ref, exit_ref, dv_ref, dkq_ref,
    state_s, bias_s, dk_s, dv_s,
):
    step = pl.program_id(0)
    block = pl.num_programs(0) - 1 - step

    @pl.when(step == 0)
    def _():
        state_s[...] = unpack_state(exit_ref[...])

    base, cumulative, row, entering, leaving = block_parts(starts_ref, decay_ref, block)
    fill_bias(starts_ref, bias_s, base, row)
    columns = cumulative.T
    keys, queries, values = kq_ref[:, : H * NS], kq_ref[:, H * NS :], vals_ref[...]
    grads = dy_ref[...]
    low_state = state_s[...].astype(jnp.bfloat16)
    dv_s[...] = product(keys, low_state) * per_lane(leaving, P_SIZE)
    dk_s[...] = input_grad(values, low_state) * per_lane(leaving, NS)
    dq = input_grad(grads, saved_ref[0]) * per_lane(entering, NS)
    half = BLK // 2
    for quad in range(H // 4):
        lanes = slice(quad * 128, quad * 128 + 128)
        sums = [dq[:half, lanes], dq[half:, lanes]]
        for head in range(4 * quad, 4 * quad + 4):
            _, query = lanes_of(queries, head, NS)
            key, own_key = lanes_of(keys, head, NS)
            value, _ = lanes_of(values, head, P_SIZE)
            _, grad = lanes_of(grads, head, P_SIZE)
            wide = slice(head // 2 * 128, head // 2 * 128 + 128)
            for part in range(2):
                rows = slice(part * half, part * half + half)
                seen = (part + 1) * half
                within = jnp.exp(
                    columns[rows, head : head + 1]
                    - cumulative[head : head + 1, :seen]
                    + bias_s[rows, :seen]
                )
                mixed = (within * input_grad(query[rows], key[:seen])).astype(jnp.bfloat16)
                dscores = (within * input_grad(grad[rows], value[:seen])).astype(jnp.bfloat16)
                sums[part] = sums[part] + product(dscores, own_key[:seen])
                dk_s[:seen, lanes] += weight_grad(dscores, query[rows])
                dv_s[:seen, wide] += weight_grad(mixed, grad[rows])
        for part in range(2):
            dkq_ref[part * half : part * half + half, H * NS + quad * 128 : H * NS + quad * 128 + 128] = (
                sums[part].astype(jnp.bfloat16)
            )
    dkq_ref[:, : H * NS] = dk_s[...].astype(jnp.bfloat16)
    dv_ref[...] = dv_s[...].astype(jnp.bfloat16)
    spread_last = per_lane(entering, P_SIZE)[BLK - 1 :]
    state_s[...] = advance(queries, grads, (entering, spread_last), state_s[...])


def block_specs(blocks, backward):
    def turn(i):
        return blocks - 1 - i if backward else i

    return (
        pl.BlockSpec(memory_space=pltpu.SMEM),
        pl.BlockSpec((H, BLK), lambda i: (0, turn(i))),
        pl.BlockSpec((BLK, D), lambda i: (turn(i), 0)),
        pl.BlockSpec((1, H * NS, H * P_SIZE), lambda i: (turn(i), 0, 0)),
    )


STATE = (H * NS, H * P_SIZE)
BIG = pltpu.CompilerParams(vmem_limit_bytes=48 << 20)


def state_summary(places, decays, key_query, values, backward):
    blocks = key_query.shape[0] // BLK
    scalars, heads, rows, _ = block_specs(blocks, backward)
    return pl.pallas_call(
        functools.partial(summary_kernel, backward),
        grid=(blocks,),
        out_shape=jax.ShapeDtypeStruct((144, 128), jnp.bfloat16),
        in_specs=[scalars, heads, rows, rows],
        out_specs=pl.BlockSpec((144, 128), lambda i: (0, 0)),
        scratch_shapes=[pltpu.VMEM(STATE, jnp.float32), pltpu.VMEM((H, 128), jnp.float32)],
        compiler_params=BIG,
    )(places, decays, key_query, values)


def mix_states(places, decays, key_query, values, entry):
    frames = key_query.shape[0]
    blocks = frames // BLK
    scalars, heads, rows, states = block_specs(blocks, False)
    return pl.pallas_call(
        mixing_kernel,
        grid=(blocks,),
        out_shape=(
            jax.ShapeDtypeStruct((frames, D), jnp.bfloat16),
            jax.ShapeDtypeStruct((blocks, *STATE), jnp.bfloat16),
        ),
        in_specs=[scalars, heads, rows, rows, pl.BlockSpec((128, 128), lambda i: (0, 0))],
        out_specs=(rows, states),
        scratch_shapes=[pltpu.VMEM(STATE, jnp.float32), pltpu.VMEM((BLK, BLK), jnp.float32)],
        compiler_params=BIG,
    )(places, decays, key_query, values, entry)


def unmix_states(places, decays, key_query, values, grad_y, saved, leaving_grad):
    frames = key_query.shape[0]
    blocks = frames // BLK
    scalars, heads, rows, states = block_specs(blocks, True)
    return pl.pallas_call(
        unmixing_kernel,
        grid=(blocks,),
        out_shape=(
            jax.ShapeDtypeStruct((frames, D), jnp.bfloat16),
            jax.ShapeDtypeStruct((frames, D), jnp.bfloat16),
        ),
        in_specs=[scalars, heads, rows, rows, rows, states, pl.BlockSpec((128, 128), lambda i: (0, 0))],
        out_specs=(rows, rows),
        scratch_shapes=[
            pltpu.VMEM(STATE, jnp.float32),
            pltpu.VMEM((BLK, BLK), jnp.float32),
            pltpu.VMEM((BLK, H * NS), jnp.float32),
            pltpu.VMEM((BLK, D), jnp.float32),
        ],
        compiler_params=BIG,
    )(places, decays, key_query, values, grad_y, saved, leaving_grad)


def entry_of(summary, scales):
    count = lax.axis_size("tm")
    place = lax.axis_index("tm")
    backward = scales is not None
    arrived = lax.all_gather(summary, "tm")
    if not backward:
        scales = arrived[:, 128 : 128 + H, 0].astype(jnp.float32)
    source = jnp.arange(count)[:, None]
    between = jnp.arange(count)[None, :]
    if backward:
        passed = (between < source) & (between > place)
        ahead = source > place
    else:
        passed = (between > source) & (between < place)
        ahead = source < place
    weights = jnp.prod(jnp.where(passed[:, :, None], scales[None], 1.0), axis=1)
    weights = jnp.where(ahead, weights, 0.0).reshape(count, 2, H // 2)
    weights = jnp.repeat(weights.transpose(0, 2, 1), NS, axis=1)
    weights = jnp.repeat(weights, P_SIZE, axis=2)
    return jnp.sum(weights * arrived[:, :128].astype(jnp.float32), axis=0), scales


def local(
    inputs,
    cotangent,
    frame_mask,
    slot_lengths,
    decays,
    tile_slots,
    master_weight_tiles,
    tile_first,
    tile_second,
    vector_master,
    vector_first,
    vector_second,
):
    own_rows, capacity, _ = master_weight_tiles.shape
    owners_count = lax.axis_size("utt")
    low_master = master_weight_tiles.transpose(1, 0, 2).astype(jnp.bfloat16)
    gathered = gather_tiles(low_master, tile_slots)
    w_values, w_states, w_output, w_linear, w_gate, w_project = [
        gathered[:, 16 + number].reshape(D, D) for number in range(6)
    ]
    norm_gains = vector_master[0:6]
    norm_shifts = vector_master[6:12]
    conv_taps = vector_master[12:]
    frames = inputs.shape[1]
    first_frame = lax.axis_index("tm") * frames
    starts = jnp.cumsum(slot_lengths[0]) - slot_lengths[0]

    def segment_of(positions):
        return jnp.sum((starts[None, :] <= positions[:, None]).astype(jnp.int32), axis=1) - 1

    positions = first_frame + jnp.arange(frames, dtype=jnp.int32)
    segments = segment_of(positions)
    after_a, raw_vals, key_query = ffn_first(inputs[0], gathered, vector_master)
    live_mask = frame_mask[0].astype(jnp.bfloat16)[:, None]
    state_vals = raw_vals * live_mask
    places = jnp.concatenate([starts, jnp.reshape(first_frame, (1,))]).astype(jnp.int32)
    summary = state_summary(places, decays[0], key_query, state_vals, False)
    entry_state, all_scales = entry_of(summary, None)
    low_y, saved_states = mix_states(places, decays[0], key_query, state_vals, entry_state)
    after_b = after_a + product(low_y, w_output)
    normed_c_out, unit_c, inverse_c = layer_norm(after_b, norm_gains[2], norm_shifts[2])
    low_c = normed_c_out.astype(jnp.bfloat16)
    part_lin = product(low_c, w_linear)
    part_gate = product(low_c, w_gate)
    gate_sigmoid = jax.nn.sigmoid(part_gate)
    glu_low = (part_lin * gate_sigmoid).astype(jnp.bfloat16)
    half_width = K // 2
    padded = padded_2(glu_low, (("tm", 0),), half_width)
    pad_positions = first_frame - half_width + jnp.arange(frames + 2 * half_width, dtype=jnp.int32)
    pad_segments = segment_of(pad_positions)
    tap_masks = [
        (pad_segments[kernel_offset : kernel_offset + frames] == segments).astype(jnp.float32)[
            :, None
        ]
        for kernel_offset in range(K)
    ]
    conv_sum = jnp.zeros((frames, D), jnp.float32)
    for kernel_offset in range(K):
        conv_sum = (
            conv_sum
            + conv_taps[kernel_offset]
            * padded[kernel_offset : kernel_offset + frames].astype(jnp.float32)
            * tap_masks[kernel_offset]
        )
    normed_d, unit_d, inverse_d = layer_norm(conv_sum, norm_gains[3], norm_shifts[3])
    low_d = (normed_d * jax.nn.sigmoid(normed_d)).astype(jnp.bfloat16)
    after_c = after_b + product(low_d, w_project)
    output, grad_c, tile_grads_e, vec_e = ffn_second(
        after_c, cotangent[0], gathered, vector_master, own_rows
    )
    output = output[None]
    gain_e, shift_e, gain_f, shift_f = vec_e[0], vec_e[1], vec_e[2], vec_e[3]
    project_in = grad_c.astype(jnp.bfloat16)
    grad_project = weight_grad(low_d, project_in)
    grad_swish = input_grad(project_in, w_project) * swish_slope(normed_d)
    grad_conv, gain_d, shift_d = norm_grad(grad_swish, unit_d, inverse_d, norm_gains[3])
    low_grad_conv = grad_conv.astype(jnp.bfloat16)
    grad_padded = padded_2(low_grad_conv, (("tm", 0),), half_width)
    grad_conv_wide = low_grad_conv.astype(jnp.float32)
    grad_glu = jnp.zeros((frames, D), jnp.float32)
    tap_grads = []
    for kernel_offset in range(K):
        back_start = 2 * half_width - kernel_offset
        grad_glu = (
            grad_glu
            + conv_taps[kernel_offset]
            * grad_padded[back_start : back_start + frames].astype(jnp.float32)
            * tap_masks[K - 1 - kernel_offset]
        )
        tap_grads.append(
            jnp.sum(
                grad_conv_wide
                * padded[kernel_offset : kernel_offset + frames].astype(jnp.float32)
                * tap_masks[kernel_offset],
                axis=0,
            )
        )
    grad_lin = (grad_glu * gate_sigmoid).astype(jnp.bfloat16)
    grad_gate = (grad_glu * part_lin * gate_sigmoid * (1.0 - gate_sigmoid)).astype(jnp.bfloat16)
    grad_w_linear = weight_grad(low_c, grad_lin)
    grad_w_gate = weight_grad(low_c, grad_gate)
    grad_in_c, gain_c, shift_c = norm_grad(
        input_grad(grad_lin, w_linear) + input_grad(grad_gate, w_gate),
        unit_c,
        inverse_c,
        norm_gains[2],
    )
    grad_b = grad_c + grad_in_c
    output_in = grad_b.astype(jnp.bfloat16)
    grad_w_output = weight_grad(low_y, output_in)
    grad_y = input_grad(output_in, w_output).astype(jnp.bfloat16)
    summary = state_summary(places, decays[0], key_query, grad_y, True)
    exit_grad, _ = entry_of(summary, all_scales)
    grad_v_low, grad_kq_low = unmix_states(
        places, decays[0], key_query, state_vals, grad_y, saved_states, exit_grad
    )
    grad_v_low = grad_v_low * live_mask
    low_b = layer_norm(after_a, norm_gains[1], norm_shifts[1])[0].astype(jnp.bfloat16)
    grad_w_values = weight_grad(low_b, grad_v_low)
    grad_w_states = weight_grad(low_b, grad_kq_low)
    _, unit_b, inverse_b = layer_norm(after_a, norm_gains[1], norm_shifts[1])
    grad_in_b, gain_b, shift_b = norm_grad(
        input_grad(grad_v_low, w_values) + input_grad(grad_kq_low, w_states),
        unit_b,
        inverse_b,
        norm_gains[1],
    )
    grad_a = grad_b + grad_in_b
    count = lax.axis_size("tm")
    shards_e = halving_sum(tile_grads_e.reshape(count, 8 * own_rows, D), "tm")
    grad_a, shards_e = lax.optimization_barrier((grad_a, shards_e))
    grad_start, tile_grads_a, vec_a = ffn_back(
        inputs[0], grad_a, gathered, vector_master, own_rows
    )
    gain_a, shift_a = vec_a[0], vec_a[1]
    vector_grad = jnp.concatenate(
        [
            jnp.stack(
                [
                    gain_a,
                    gain_b,
                    gain_c,
                    gain_d,
                    gain_e,
                    gain_f,
                    shift_a,
                    shift_b,
                    shift_c,
                    shift_d,
                    shift_e,
                    shift_f,
                ]
            ),
            jnp.stack(tap_grads),
        ],
        axis=0,
    )
    mixers = jnp.stack(
        [grad_w_values, grad_w_states, grad_w_output, grad_w_linear, grad_w_gate, grad_project]
    ).astype(jnp.bfloat16)
    mixers = mixers.reshape(6, count, own_rows, D).transpose(1, 0, 2, 3)
    tail = jnp.zeros((VEC_ROWS - vector_grad.shape[0], D), jnp.float32)
    vectors = jnp.concatenate([vector_grad, tail], axis=0).astype(jnp.bfloat16)
    shards_m = halving_sum(mixers.reshape(count, 6 * own_rows, D), "tm")
    shards_a = halving_sum(
        jnp.concatenate(
            [
                tile_grads_a.reshape(count, 8 * own_rows, D),
                jnp.broadcast_to(vectors[None], (count, VEC_ROWS, D)),
            ],
            axis=1,
        ),
        "tm",
    )
    shards = jnp.concatenate(
        [
            shards_a[: 8 * own_rows].reshape(8, own_rows, D),
            shards_m.reshape(6, own_rows, D),
            shards_e.reshape(8, own_rows, D),
            jnp.zeros((1, own_rows, D), jnp.bfloat16),
        ],
        axis=0,
    )
    tiles = tile_slots.shape[0]
    tile_of = (
        jnp.full((owners_count * capacity,), tiles, jnp.int32)
        .at[tile_slots]
        .set(jnp.arange(tiles, dtype=jnp.int32))
    )
    placed = shards[tile_of].reshape(owners_count, capacity * own_rows, D)
    shared = jnp.broadcast_to(shards_a[None, 8 * own_rows :], (owners_count, VEC_ROWS, D))
    reduced = lax.psum_scatter(
        jnp.concatenate([placed, shared], axis=1), "utt", scatter_dimension=0
    ).astype(jnp.float32)
    vector_total = reduced[capacity * own_rows :][: vector_grad.shape[0]]
    reduced = reduced[: capacity * own_rows].reshape(capacity, own_rows, D).transpose(1, 0, 2)
    tile_new, first_new, second_new = adam_step(
        master_weight_tiles, tile_first, tile_second, reduced, RATE_TILES, DECAY_TILES
    )
    vector_new, vfirst_new, vsecond_new = adam_step(
        vector_master, vector_first, vector_second, vector_total, RATE_VECTORS, 0.0
    )
    return (
        output,
        grad_start[None],
        tile_new,
        first_new,
        second_new,
        tile_new.astype(jnp.bfloat16),
        vector_new,
        vfirst_new,
        vsecond_new,
    )


def solution(mesh):
    in_specs = (
        P("utt", "tm", None),
        P("utt", "tm", None),
        P("utt", "tm"),
        P("utt", None),
        P("utt", None, "tm"),
        P(),
        P(("utt", "tm"), None, None),
        P(("utt", "tm"), None, None),
        P(("utt", "tm"), None, None),
        P(),
        P(),
        P(),
    )
    out_specs = (
        P("utt", "tm", None),
        P("utt", "tm", None),
        P(("utt", "tm"), None, None),
        P(("utt", "tm"), None, None),
        P(("utt", "tm"), None, None),
        P(("utt", "tm"), None, None),
        P(),
        P(),
        P(),
    )
    return jax.shard_map(local, mesh=mesh, in_specs=in_specs, out_specs=out_specs, check_vma=False)
```
